128 devices in a mesh: data: 64 (over z, y, x), stage: 2 (over core).
Axes of the slice: x: 4, y: 4, z: 4, core: 2. Of those that a mesh axis runs over, the one named last changes fastest.
Arguments:
- x: bfloat16 [8, 128, 32, 1024], P(None, 'data')
- g: bfloat16 [8, 128, 32, 1024], P(None, 'data')
- w_gate: bfloat16 [2, 1, 1024, 4096], P('stage', None, 'data')
- w_in: bfloat16 [2, 1, 1024, 4096], P('stage', None, 'data')
- w_out: bfloat16 [2, 1, 4096, 1024], P('stage', None, 'data')
Outputs:
- output 1: bfloat16 [8, 128, 32, 1024], P(None, 'data')
- output 2: float32 [2, 1, 1024, 4096], P('stage', None, 'data')
- output 3: float32 [2, 1, 1024, 4096], P('stage', None, 'data')
- output 4: float32 [2, 1, 4096, 1024], P('stage', None, 'data')
All inputs are finite; a program needn't handle non-finite values.
Results may differ from the reference program's by a relative error of at most 0.0116991.
Values are sent between devices in bfloat16 or wider.
A program may use at most 1 GiB of HBM per device.

```python
import jax
import jax.numpy as jnp
from jax import lax

NUM_STAGES = 2
DATA_DEVS = 64
NUM_MICRO = 8
BATCH_MB = 2
SEQ_LEN = 32
LAYERS = 1
DMODEL = 1024
FFN_DIM = 4096


def setup_inputs(seed: int = 0) -> dict:
    rng_key = jax.random.key(seed)
    sub_keys = jax.random.split(rng_key, 5)
    act_shape = (NUM_MICRO, DATA_DEVS * BATCH_MB, SEQ_LEN, DMODEL)
    up_shape = (NUM_STAGES, LAYERS, DMODEL, FFN_DIM)
    down_shape = (NUM_STAGES, LAYERS, FFN_DIM, DMODEL)
    x = jax.random.normal(sub_keys[0], act_shape, jnp.float32).astype(jnp.bfloat16)
    g = jax.random.normal(sub_keys[1], act_shape, jnp.float32).astype(jnp.bfloat16)
    w_gate = (jax.random.normal(sub_keys[2], up_shape, jnp.float32) * DMODEL ** -0.5).astype(jnp.bfloat16)
    w_in = (jax.random.normal(sub_keys[3], up_shape, jnp.float32) * DMODEL ** -0.5).astype(jnp.bfloat16)
    w_out = (jax.random.normal(sub_keys[4], down_shape, jnp.float32) * FFN_DIM ** -0.5).astype(jnp.bfloat16)
    return {'x': x, 'g': g, 'w_gate': w_gate, 'w_in': w_in, 'w_out': w_out}


def rms_f32(row_vals):
    return row_vals * lax.rsqrt(jnp.mean(row_vals * row_vals, axis=-1, keepdims=True) + 1e-6)


def layer_fwd(tokens, w_gate, w_in, w_out):
    normed = rms_f32(tokens.astype(jnp.float32)).astype(jnp.bfloat16)
    pre_gate = jnp.dot(normed, w_gate, preferred_element_type=jnp.float32)
    pre_in = jnp.dot(normed, w_in, preferred_element_type=jnp.float32)
    hidden = (pre_gate * jax.nn.sigmoid(pre_gate) * pre_in).astype(jnp.bfloat16)
    branch = jnp.dot(hidden, w_out, preferred_element_type=jnp.float32)
    return tokens + branch.astype(jnp.bfloat16)


def layer_bwd(tokens, d_next, w_gate, w_in, w_out):
    normed_f, rms_pull = jax.vjp(rms_f32, tokens.astype(jnp.float32))
    normed = normed_f.astype(jnp.bfloat16)
    pre_gate = jnp.dot(normed, w_gate, preferred_element_type=jnp.float32)
    pre_in = jnp.dot(normed, w_in, preferred_element_type=jnp.float32)
    sigma_gate = jax.nn.sigmoid(pre_gate)
    gate_act = pre_gate * sigma_gate
    hidden = (gate_act * pre_in).astype(jnp.bfloat16)
    d_wout = jnp.dot(hidden.T, d_next, preferred_element_type=jnp.float32)
    d_hidden = jnp.dot(d_next, w_out.T, preferred_element_type=jnp.float32)
    d_gate = (d_hidden * pre_in * sigma_gate * (1.0 + pre_gate * (1.0 - sigma_gate))).astype(jnp.bfloat16)
    d_up = (d_hidden * gate_act).astype(jnp.bfloat16)
    d_wgate = jnp.dot(normed.T, d_gate, preferred_element_type=jnp.float32)
    d_win = jnp.dot(normed.T, d_up, preferred_element_type=jnp.float32)
    d_normed = jnp.dot(d_gate, w_gate.T, preferred_element_type=jnp.float32) + jnp.dot(d_up, w_in.T, preferred_element_type=jnp.float32)
    d_resid = rms_pull(d_normed)[0]
    d_prev = (d_next.astype(jnp.float32) + d_resid).astype(jnp.bfloat16)
    return d_prev, d_wgate, d_win, d_wout


def reference(x, g, w_gate, w_in, w_out):
    n_blocks = NUM_STAGES * LAYERS
    gate_all = w_gate.reshape(n_blocks, DMODEL, FFN_DIM)
    in_all = w_in.reshape(n_blocks, DMODEL, FFN_DIM)
    out_all = w_out.reshape(n_blocks, FFN_DIM, DMODEL)

    def one_micro(grad_sums, micro_pair):
        x_micro = micro_pair[0]
        g_micro = micro_pair[1]

        def fwd_step(tokens, weights):
            return layer_fwd(tokens, weights[0], weights[1], weights[2]), tokens

        _, block_inputs = lax.scan(fwd_step, x_micro.reshape(-1, DMODEL), (gate_all, in_all, out_all))

        def bwd_step(d_next, block_items):
            d_prev, d_wgate, d_win, d_wout = layer_bwd(block_items[0], d_next, block_items[1], block_items[2], block_items[3])
            return d_prev, (d_wgate, d_win, d_wout)

        d_first, block_grads = lax.scan(bwd_step, g_micro.reshape(-1, DMODEL), (block_inputs, gate_all, in_all, out_all), reverse=True)
        new_sums = (grad_sums[0] + block_grads[0], grad_sums[1] + block_grads[1], grad_sums[2] + block_grads[2])
        return new_sums, d_first.reshape(x_micro.shape)

    zero_up = jnp.zeros((n_blocks, DMODEL, FFN_DIM), jnp.float32)
    zero_down = jnp.zeros((n_blocks, FFN_DIM, DMODEL), jnp.float32)
    grad_sums, d_x = lax.scan(one_micro, (zero_up, zero_up, zero_down), (x, g))
    return (d_x, grad_sums[0].reshape(w_gate.shape), grad_sums[1].reshape(w_in.shape), grad_sums[2].reshape(w_out.shape))
```

```python
import functools

import jax
import jax.numpy as jnp
from jax import lax
from jax.experimental import pallas as pl
from jax.experimental.pallas import tpu as pltpu
from jax.sharding import PartitionSpec as P

MESH = pl.DeviceIdType.MESH
BF16 = jnp.bfloat16
F32 = jnp.float32
RING = 4
HALF = 128
STEP = 16
WIDE = 1024


class Place:
    def __init__(self, ssem, rsem, lsem):
        d = lax.axis_index('data')
        self.c = c = lax.axis_index('stage')
        self.z = z = d // 16
        self.y = y = (d // 4) % 4
        self.x = x = d % 4
        self.ssem, self.rsem, self.lsem = ssem, rsem, lsem
        self.n_slots = self.n_local = 0
        self.a1, self.a2 = self.order(y, x, c)
        self.z_ring = (z, self.dev((z + 1) % 4, y, x, c), self.dev((z + 3) % 4, y, x, c))
        k = 1 - c
        self.ring1 = (self.a1, self.dev(z, (y + c) % 4, (x + k) % 4, c), self.dev(z, (y + 3 * c) % 4, (x + 3 * k) % 4, c))
        self.ring2 = (self.a2, self.dev(z, (y + k) % 4, (x + c) % 4, c), self.dev(z, (y + 3 * k) % 4, (x + 3 * c) % 4, c))
        self.partner = self.dev(z, y, x, 1 - c)

    @staticmethod
    def order(y, x, c):
        return (1 - c) * x + c * y, (1 - c) * y + c * x

    @staticmethod
    def dev(z, y, x, c):
        return (z * 16 + y * 4 + x, c)

    def slot(self):
        self.n_slots += 1
        return self.n_slots - 1

    def local_slot(self):
        self.n_local += 1
        return self.n_local - 1

    def remote(self, src, dst, dev, slot):
        return pltpu.make_async_remote_copy(src_ref=src, dst_ref=dst, send_sem=self.ssem.at[slot], recv_sem=self.rsem.at[slot], device_id=dev, device_id_type=MESH)

    def push(self, src, dst, dev):
        copy = self.remote(src, dst, dev, self.slot())
        copy.start()
        return copy

    def barrier(self):
        sem = pltpu.get_barrier_semaphore()
        z, y, x, c = self.z, self.y, self.x, self.c
        peers = [self.partner]
        for dz in range(1, 4):
            peers.append(self.dev((z + dz) % 4, y, x, c))
            peers.append(self.dev((z + dz) % 4, y, x, 1 - c))
        peers += [self.ring1[1], self.ring1[2], self.ring2[1], self.ring2[2]]
        for peer in peers:
            pl.semaphore_signal(sem, inc=1, device_id=peer, device_id_type=MESH)
        pl.semaphore_wait(sem, len(peers))


class Gather:
    def __init__(self, place, ring, at):
        self.pl, self.at = place, at
        self.me, self.plus, self.minus = ring

    def start(self):
        me, at, push = self.me, self.at, self.pl.push
        self.p0 = push(at(me, 0), at(me, 0), self.plus)
        self.m1 = push(at(me, 1), at(me, 1), self.minus)
        self.p1 = push(at(me, 1), at(me, 1), self.plus)
        self.m0 = push(at(me, 0), at(me, 0), self.minus)
        return self

    def relay(self):
        before, after = (self.me + 3) % 4, (self.me + 1) % 4
        self.p0.wait_recv()
        self.rp = self.pl.push(self.at(before, 0), self.at(before, 0), self.plus)
        self.m1.wait_recv()
        self.rm = self.pl.push(self.at(after, 1), self.at(after, 1), self.minus)

    def finish(self):
        for copy in (self.p1, self.m0, self.rp, self.rm):
            copy.wait_recv()
        for copy in (self.p0, self.m1, self.p1, self.m0, self.rp, self.rm):
            copy.wait_send()


class Reduce:
    def __init__(self, place, ring, own, held, add):
        self.pl, self.own, self.held, self.add = place, own, held, add
        self.me, self.plus, self.minus = ring

    def start(self):
        me, own, push = self.me, self.own, self.pl.push
        relay, left, right = self.held
        far, after, before = (me + 2) % 4, (me + 1) % 4, (me + 3) % 4
        self.a = push(own(far, 0), relay.at[0], self.plus)
        self.b = push(own(far, 1), relay.at[1], self.minus)
        self.c = push(own(after, 1), left.at[1], self.plus)
        self.d = push(own(before, 0), right.at[0], self.minus)
        return self

    def relay(self):
        relay, left, right = self.held
        after, before = (self.me + 1) % 4, (self.me + 3) % 4
        self.a.wait_recv()
        self.add(relay, 0, after)
        self.e = self.pl.push(relay.at[0], left.at[0], self.plus)
        self.b.wait_recv()
        self.add(relay, 1, before)
        self.f = self.pl.push(relay.at[1], right.at[1], self.minus)

    def finish(self):
        for copy in (self.c, self.d, self.e, self.f):
            copy.wait_recv()
        for copy in (self.a, self.b, self.c, self.d, self.e, self.f):
            copy.wait_send()


def rows_of(i):
    return pl.ds(pl.multiple_of(i * STEP, STEP), STEP)


def by_rows(body):
    for h in range(2):
        def one(i, carry, h=h):
            body(h, rows_of(i))
            return carry
        lax.fori_loop(0, HALF // STEP, one, 0)


def inverse_rms(rows):
    return lax.rsqrt(jnp.mean(rows * rows, axis=-1, keepdims=True) + 1e-6)


def rms(rows):
    return (rows * inverse_rms(rows)).astype(BF16)


def cotangent(h, e, dn):
    r = inverse_rms(h)
    back = r * dn - h * (r * r * r * jnp.mean(h * dn, axis=-1, keepdims=True))
    return (e + back).astype(BF16)


def row_reduce(place, part, held):
    def add(dst, h, j):
        def one(i, carry):
            rows = rows_of(i)
            dst[h, rows] = dst[h, rows] + part[j, h, rows]
            return carry
        lax.fori_loop(0, HALF // STEP, one, 0)
    return Reduce(place, place.z_ring, lambda j, h: part.at[j, h], held, add)


def row_sum(place, part, held, h, rows):
    return part[place.z, h, rows] + held[1][h, rows] + held[2][h, rows]


class Weights:
    def __init__(self, place, s, shards, held, outs):
        self.pl, self.s, self.shards, self.held, self.outs = place, s, shards, held, outs
        self.slots = [[place.slot() for _ in range(2)] for _ in range(4)]
        self.out_slot = place.slot()
        self.swap_slots = [place.slot() for _ in range(3)]
        self.local = [place.local_slot() for _ in range(3)]
        self.copy_local = [place.local_slot() for _ in range(3)]

    def parts(self, dz):
        place = self.pl
        target = (place.z + dz) % 4
        core = place.z // 2
        a1, a2 = place.order(place.y, place.x, core)
        cols = pl.ds(pl.multiple_of(target * WIDE, WIDE), WIDE)
        for m in range(2):
            yield m, self.shards[m].at[:, cols], self.held.at[a1, a2, place.z % 2, m], place.dev(target, place.y, place.x, core)

    def out_part(self, core):
        a1, a2 = self.pl.order(self.pl.y, self.pl.x, core)
        return self.shards[2].at[2 * core:2 * core + 2], self.held.at[a1, a2, :, 2]

    def send(self):
        place, s = self.pl, self.s
        mine = place.z // 2 == s

        @pl.when(place.c == s)
        def _():
            for dz in range(1, 4):
                for m, src, dst, dev in self.parts(dz):
                    place.remote(src, dst, dev, self.slots[dz][m]).start()

            @pl.when(mine)
            def _():
                for m, src, dst, _ in self.parts(0):
                    pltpu.make_async_copy(src, dst, place.lsem.at[self.local[m]]).start()

            @pl.when(jnp.logical_not(mine))
            def _():
                for m, src, dst, _ in self.parts(0):
                    place.remote(src, dst, place.partner, self.slots[0][m]).start()
            src, dst = self.out_part(s)
            pltpu.make_async_copy(src, dst, place.lsem.at[self.local[2]]).start()
            src, dst = self.out_part(1 - s)
            place.remote(src, dst, place.partner, self.out_slot).start()

    def arrive(self):
        place, s = self.pl, self.s
        is_source = place.c == s
        mine = place.z // 2 == s
        for dz in range(4):
            source = (place.z + 4 - dz) % 4
            here = source // 2 == place.c
            if dz == 0:
                here = jnp.logical_and(here, jnp.logical_not(is_source))

            @pl.when(here)
            def _(dz=dz, source=source):
                for m in range(2):
                    dst = self.held.at[place.a1, place.a2, source % 2, m]
                    place.remote(dst, dst, place.partner, self.slots[dz][m]).wait_recv()

        @pl.when(is_source)
        def _():
            for dz in range(1, 4):
                for m, src, dst, dev in self.parts(dz):
                    place.remote(src, dst, dev, self.slots[dz][m]).wait_send()

            @pl.when(mine)
            def _():
                for m, src, dst, _ in self.parts(0):
                    pltpu.make_async_copy(src, dst, place.lsem.at[self.local[m]]).wait()

            @pl.when(jnp.logical_not(mine))
            def _():
                for m, src, dst, _ in self.parts(0):
                    place.remote(src, dst, place.partner, self.slots[0][m]).wait_send()
            src, dst = self.out_part(s)
            pltpu.make_async_copy(src, dst, place.lsem.at[self.local[2]]).wait()
            src, dst = self.out_part(1 - s)
            place.remote(src, dst, place.partner, self.out_slot).wait_send()

        @pl.when(jnp.logical_not(is_source))
        def _():
            _, dst = self.out_part(1 - s)
            place.remote(dst, dst, place.partner, self.out_slot).wait_recv()

    def first(self):
        place, held = self.pl, self.held
        return Gather(place, place.ring2, lambda j, h: held.at[place.a1, j, h]).start()

    def second(self):
        place, held = self.pl, self.held
        return Gather(place, place.ring1, lambda j, h: held.at[j, 2 * h:2 * h + 2]).start()

    def place_of(self, m, p, core):
        if m < 2:
            return self.outs[m].at[pl.ds(2 * core, 2), p]
        return self.outs[m].at[p, pl.ds(2 * core, 2)]

    def half_of(self, m, core):
        if m < 2:
            return self.outs[m].at[pl.ds(2 * core, 2)]
        return self.outs[m].at[:, pl.ds(2 * core, 2)]

    def spread(self):
        place = self.pl

        def one(p, carry):
            a1, a2 = place.order(p // 4, p % 4, place.c)
            for m in range(3):
                src = self.held.at[a1, a2, :, m]
                dst = self.place_of(m, p, place.c)
                place.remote(src, dst, place.partner, self.swap_slots[m]).start()
                pltpu.make_async_copy(src, dst, place.lsem.at[self.copy_local[m]]).start()
            return carry
        lax.fori_loop(0, 16, one, 0)

    def done(self):
        place = self.pl
        for m in range(3):
            mine, other = self.half_of(m, place.c), self.half_of(m, 1 - place.c)
            place.remote(mine, other, place.partner, self.swap_slots[m]).wait_recv()
            place.remote(mine, other, place.partner, self.swap_slots[m]).wait_send()
            pltpu.make_async_copy(mine, mine, place.lsem.at[self.copy_local[m]]).wait()


class Grads:
    def __init__(self, place, s, parts, mine, held1, sum1, held2, sum2, outs):
        self.pl, self.s, self.parts, self.mine = place, s, parts, mine
        self.held1, self.sum1, self.held2, self.sum2, self.outs = held1, sum1, held2, sum2, outs
        self.swap_slots = [place.slot() for _ in range(3)]
        self.slots = [[place.slot() for _ in range(2)] for _ in range(4)]
        self.out_slot = place.slot()
        self.local = [place.local_slot() for _ in range(3)]

    def part(self, m, p, core):
        if m < 2:
            return self.parts[m].at[pl.ds(2 * core, 2), p]
        return self.parts[m].at[p, pl.ds(2 * core, 2)]

    def swap(self):
        place = self.pl

        def one(p, carry):
            other = 1 - place.c
            a1, a2 = place.order(p // 4, p % 4, other)
            for m in range(3):
                place.remote(self.part(m, p, other), self.mine.at[a1, a2, :, m], place.partner, self.swap_slots[m]).start()
            return carry
        lax.fori_loop(0, 16, one, 0)

    def combine(self):
        place, mine = self.pl, self.mine
        for m in range(3):
            whole = mine.at[:, :, :, m]
            place.remote(whole, whole, place.partner, self.swap_slots[m]).wait_recv()

        def one(p, carry):
            a1, a2 = place.order(p // 4, p % 4, place.c)
            for q in range(2):
                for m in range(3):
                    own = self.parts[m][2 * place.c + q, p] if m < 2 else self.parts[m][p, 2 * place.c + q]
                    mine[a1, a2, q, m] = mine[a1, a2, q, m] + own
            return carry
        lax.fori_loop(0, 16, one, 0)
        for m in range(3):
            whole = mine.at[:, :, :, m]
            place.remote(whole, whole, place.partner, self.swap_slots[m]).wait_send()

    def first(self):
        place, mine = self.pl, self.mine

        def add(dst, h, j):
            def one(i, carry):
                k, q = i // 2, i % 2
                for m in range(3):
                    dst[h, k, q, m] = dst[h, k, q, m] + mine[j, 2 * h + k, q, m]
                return carry
            lax.fori_loop(0, 4, one, 0)
        return Reduce(place, place.ring1, lambda j, h: mine.at[j, 2 * h:2 * h + 2], self.held1, add).start()

    def first_sum(self):
        place, mine = self.pl, self.mine
        for h in range(2):
            def one(i, carry, h=h):
                k, q = i // 2, i % 2
                for m in range(3):
                    total = mine[place.a1, 2 * h + k, q, m] + self.held1[1][h, k, q, m] + self.held1[2][h, k, q, m]
                    self.sum1[2 * h + k, q, m] = total
                return carry
            lax.fori_loop(0, 4, one, 0)

    def second(self):
        place, sum1 = self.pl, self.sum1

        def add(dst, h, j):
            for m in range(3):
                dst[h, m] = dst[h, m] + sum1[j, h, m]
        return Reduce(place, place.ring2, lambda j, h: sum1.at[j, h], self.held2, add).start()

    def second_sum(self):
        place = self.pl
        for h in range(2):
            for m in range(3):
                self.sum2[h, m] = self.sum1[place.a2, h, m] + self.held2[1][h, m] + self.held2[2][h, m]

    def shard(self, m, source):
        return self.outs[m].at[:, pl.ds(pl.multiple_of(source * WIDE, WIDE), WIDE)]

    def hand(self, wait):
        place, s = self.pl, self.s
        for dz in range(4):
            target = (place.z + dz) % 4
            to_self = place.c == s

            def go(dz=dz, target=target):
                for m in range(2):
                    copy = place.remote(self.sum2.at[target % 2, m], self.shard(m, place.z), place.dev(target, place.y, place.x, s), self.slots[dz][m])
                    copy.wait_send() if wait else copy.start()

            here = target // 2 == place.c
            if dz:
                pl.when(here)(go)
                continue

            def stay():
                for m in range(2):
                    copy = pltpu.make_async_copy(self.sum2.at[place.z % 2, m], self.shard(m, place.z), place.lsem.at[self.local[m]])
                    copy.wait() if wait else copy.start()
            pl.when(jnp.logical_and(here, to_self))(stay)
            pl.when(jnp.logical_and(here, jnp.logical_not(to_self)))(go)

        rows = self.outs[2].at[pl.ds(2 * place.c, 2)]

        @pl.when(place.c == s)
        def _():
            copy = pltpu.make_async_copy(self.sum2.at[:, 2], rows, place.lsem.at[self.local[2]])
            copy.wait() if wait else copy.start()

        @pl.when(place.c != s)
        def _():
            copy = place.remote(self.sum2.at[:, 2], rows, place.partner, self.out_slot)
            copy.wait_send() if wait else copy.start()

    def done(self):
        place, s = self.pl, self.s

        @pl.when(place.c == s)
        def _():
            for dz in range(4):
                def land(dz=dz):
                    for m in range(2):
                        dst = self.shard(m, (place.z + 4 - dz) % 4)
                        place.remote(dst, dst, place.partner, self.slots[dz][m]).wait_recv()
                if dz:
                    land()
                else:
                    pl.when(place.z // 2 != s)(land)
            dst = self.outs[2].at[pl.ds(2 * (1 - place.c), 2)]
            place.remote(dst, dst, place.partner, self.out_slot).wait_recv()
        self.hand(True)


def kernel_a(x_ref, g_ref, wg, wi, wo, n_ref, ga_ref, og, oi, oo, held_w, ssem, rsem, lsem):
    place = Place(ssem, rsem, lsem)
    place.barrier()
    weights = Weights(place, 0, (wg, wi, wo), held_w, (og, oi, oo))
    weights.send()
    z, c = place.z, place.c
    g_copy = pltpu.make_async_copy(g_ref.at[c], ga_ref.at[z], lsem.at[place.local_slot()])
    g_copy.start()

    def norm(h, rows):
        n_ref[z, h, rows] = rms(x_ref[c, h, rows].astype(F32))
    by_rows(norm)
    rows_n = Gather(place, place.z_ring, lambda j, h: n_ref.at[j, h]).start()
    weights.arrive()
    w_first = weights.first()
    w_first.relay()
    w_first.finish()
    w_second = weights.second()
    rows_n.relay()
    g_copy.wait()
    rows_g = Gather(place, place.z_ring, lambda j, h: ga_ref.at[j, h]).start()
    w_second.relay()
    rows_n.finish()
    w_second.finish()
    weights.spread()
    rows_g.relay()
    rows_g.finish()
    weights.done()


def kernel_b(part, x_ref, wg, wi, wo, h_ref, n_ref, og, oi, oo, held, left, right, held_w, ssem, rsem, lsem):
    place = Place(ssem, rsem, lsem)
    place.barrier()
    bufs = (held, left, right)
    weights = Weights(place, 1, (wg, wi, wo), held_w, (og, oi, oo))
    weights.send()
    rows_o = row_reduce(place, part, bufs).start()
    weights.arrive()
    w_first = weights.first()
    w_first.relay()
    w_first.finish()
    w_second = weights.second()
    rows_o.relay()
    w_second.relay()
    w_second.finish()
    weights.spread()
    rows_o.finish()
    z, c = place.z, place.c

    def step(h, rows):
        o = row_sum(place, part, bufs, h, rows).astype(BF16).astype(F32)
        out = (x_ref[c, h, rows].astype(F32) + o).astype(BF16)
        h_ref[h, rows] = out
        n_ref[z, h, rows] = rms(out.astype(F32))
    by_rows(step)
    rows_n = Gather(place, place.z_ring, lambda j, h: n_ref.at[j, h]).start()
    rows_n.relay()
    rows_n.finish()
    weights.done()


def kernel_c(part, h_ref, g_ref, dg, di, do, wg, wi, wo, e_ref, eo_ref, og, oi, oo, gg, gi, go, held, left, right, held_w, mine, h1, l1, r1, sum1, h2, l2, r2, sum2, ssem, rsem, lsem):
    place = Place(ssem, rsem, lsem)
    place.barrier()
    bufs = (held, left, right)
    z, c = place.z, place.c
    weights = Weights(place, 0, (wg, wi, wo), held_w, (og, oi, oo))
    grads = Grads(place, 1, (dg, di, do), mine, (h1, l1, r1), sum1, (h2, l2, r2), sum2, (gg, gi, go))
    weights.send()
    rows_d = row_reduce(place, part, bufs).start()
    grads.swap()
    weights.arrive()
    w_first = weights.first()
    w_first.relay()
    w_first.finish()
    w_second = weights.second()
    grads.combine()
    g_first = grads.first()
    rows_d.relay()
    w_second.relay()
    g_first.relay()
    w_second.finish()
    weights.spread()
    rows_d.finish()

    def step(h, rows):
        dn = row_sum(place, part, bufs, h, rows)
        e = cotangent(h_ref[h, rows].astype(F32), g_ref[c, h, rows].astype(F32), dn)
        e_ref[z, h, rows] = e
        eo_ref[h, rows] = e
    by_rows(step)
    rows_e = Gather(place, place.z_ring, lambda j, h: e_ref.at[j, h]).start()
    g_first.finish()
    grads.first_sum()
    g_second = grads.second()
    rows_e.relay()
    g_second.relay()
    g_second.finish()
    grads.second_sum()
    grads.hand(False)
    rows_e.finish()
    weights.done()
    grads.done()


def kernel_d(part, x_ref, e_ref, dg, di, do, dx_ref, gg, gi, go, held, left, right, mine, h1, l1, r1, sum1, h2, l2, r2, sum2, ssem, rsem, lsem):
    place = Place(ssem, rsem, lsem)
    place.barrier()
    bufs = (held, left, right)
    c = place.c
    grads = Grads(place, 0, (dg, di, do), mine, (h1, l1, r1), sum1, (h2, l2, r2), sum2, (gg, gi, go))
    grads.swap()
    rows_d = row_reduce(place, part, bufs).start()
    grads.combine()
    g_first = grads.first()
    rows_d.relay()
    g_first.relay()
    rows_d.finish()

    def step(h, rows):
        dn = row_sum(place, part, bufs, h, rows)
        dx_ref[c, h, rows] = cotangent(x_ref[c, h, rows].astype(F32), e_ref[h, rows].astype(F32), dn)
    by_rows(step)
    swap = place.push(dx_ref.at[c], dx_ref.at[c], place.partner)
    g_first.finish()
    grads.first_sum()
    g_second = grads.second()
    g_second.relay()
    g_second.finish()
    grads.second_sum()
    grads.hand(False)
    swap.wait()
    grads.done()


VM = pl.BlockSpec(memory_space=pltpu.VMEM)
ANY = pl.BlockSpec(memory_space=pl.ANY)


def sds(shape, dtype):
    return jax.ShapeDtypeStruct(shape, dtype)


ALL_ROWS = (4, 2, HALF, WIDE)
OWN_ROWS = (2, HALF, WIDE)
W_SHAPES = [sds((4, 16, 16, WIDE), BF16), sds((4, 16, 16, WIDE), BF16), sds((16, 4, 16, WIDE), BF16)]
G_SHAPES = [sds((16, 4 * WIDE), F32), sds((16, 4 * WIDE), F32), sds((4, 16, WIDE), F32)]
ROW_BUFS = [pltpu.VMEM(OWN_ROWS, F32)] * 3
W_BUFS = [pltpu.VMEM((4, 4, 2, 3, 16, WIDE), BF16)]
G_BUFS = (
    [pltpu.VMEM((4, 4, 2, 3, 16, WIDE), F32)]
    + [pltpu.VMEM((2, 2, 2, 3, 16, WIDE), F32)] * 3
    + [pltpu.VMEM((4, 2, 3, 16, WIDE), F32)]
    + [pltpu.VMEM((2, 3, 16, WIDE), F32)] * 3
    + [pltpu.VMEM((2, 3, 16, WIDE), F32)]
)
SEMS = [pltpu.SemaphoreType.DMA((64,)), pltpu.SemaphoreType.DMA((64,)), pltpu.SemaphoreType.DMA((16,))]


def call(kernel, cid, n_in, outs, out_specs, scratch):
    return pl.pallas_call(
        kernel,
        out_shape=outs,
        in_specs=[VM] * n_in,
        out_specs=out_specs,
        scratch_shapes=scratch + SEMS,
        compiler_params=pltpu.CompilerParams(collective_id=cid, has_side_effects=True, vmem_limit_bytes=60 * 1024 * 1024),
        name=kernel.__name__,
    )


def mm(a, b):
    return jnp.dot(a, b, preferred_element_type=F32)


def mm_t(a, b):
    return lax.dot_general(a, b, (((0,), (0,)), ((), ())), preferred_element_type=F32)


def mm_nt(a, b):
    return lax.dot_general(a, b, (((1,), (1,)), ((), ())), preferred_element_type=F32)


def flat(t):
    return t.reshape(-1, WIDE)


def backward(n, a, b, u, e, gate, inn, out):
    s = jax.nn.sigmoid(a)
    d_out = mm_t(u, e)
    t = mm_nt(e, out)
    da = (t * b * s * (1.0 + a * (1.0 - s))).astype(BF16)
    db = (t * (a * s)).astype(BF16)
    dn = mm_nt(da, gate) + mm_nt(db, inn)
    d_gate = mm_t(n, da)
    d_in = mm_t(n, db)
    grads = (d_gate.reshape(4, 16, 16, WIDE), d_in.reshape(4, 16, 16, WIDE), d_out.reshape(16, 4, 16, WIDE))
    return dn.reshape(ALL_ROWS), grads


def hidden(n, gate, inn):
    a, b = mm(n, gate), mm(n, inn)
    return a, b, (a * jax.nn.sigmoid(a) * b).astype(BF16)


def solution(mesh):
    act_spec = P(None, 'data', None, None)
    weight_spec = P('stage', None, 'data', None)

    def per_device(x, g, w_gate, w_in, w_out):
        xs = x.reshape(2, 2, HALF, WIDE)
        gs = g.reshape(2, 2, HALF, WIDE)
        shards = (w_gate.reshape(16, 4 * WIDE), w_in.reshape(16, 4 * WIDE), w_out.reshape(4, 16, WIDE))

        n0, g_all, *w0 = call(kernel_a, 1, 5, [sds(ALL_ROWS, BF16)] * 2 + W_SHAPES, [VM] * 2 + [ANY] * 3, W_BUFS)(xs, gs, *shards)
        n0, g_all = flat(n0), flat(g_all)
        a0, b0, u0 = hidden(n0, flat(w0[0]), flat(w0[1]))
        o0 = mm(u0, flat(w0[2])).reshape(ALL_ROWS)

        h1, n1, *w1 = call(kernel_b, 2, 5, [sds(OWN_ROWS, BF16), sds(ALL_ROWS, BF16)] + W_SHAPES, [VM] * 2 + [ANY] * 3, ROW_BUFS + W_BUFS)(o0, xs, *shards)
        n1 = flat(n1)
        w1 = [flat(w) for w in w1]
        a1, b1, u1 = hidden(n1, w1[0], w1[1])
        dn1, grads1 = backward(n1, a1, b1, u1, g_all, *w1)

        outs = [sds(ALL_ROWS, BF16), sds(OWN_ROWS, BF16)] + W_SHAPES + G_SHAPES
        e_all, e_own, *rest = call(kernel_c, 3, 9, outs, [VM] * 2 + [ANY] * 3 + [VM] * 3, ROW_BUFS + W_BUFS + G_BUFS)(dn1, h1, gs, *grads1, *shards)
        w0 = [flat(w) for w in rest[:3]]
        dn0, grads0 = backward(n0, a0, b0, u0, flat(e_all), *w0)

        outs = [sds((2, 2, HALF, WIDE), BF16)] + G_SHAPES
        dx, *own0 = call(kernel_d, 4, 6, outs, [VM] * 4, ROW_BUFS + G_BUFS)(dn0, xs, e_own, *grads0)
        first = lax.axis_index('stage') == 0
        own = [jnp.where(first, s0, s1) for s0, s1 in zip(own0, rest[3:])]
        return (dx.reshape(x.shape), own[0].reshape(w_gate.shape), own[1].reshape(w_in.shape), own[2].reshape(w_out.shape))

    return jax.shard_map(per_device, mesh=mesh, in_specs=(act_spec, act_spec, weight_spec, weight_spec, weight_spec), out_specs=(act_spec, weight_spec, weight_spec, weight_spec), check_vma=False)
```

```python
import functools

import jax
import jax.numpy as jnp
from jax import lax
from jax.experimental import pallas as pl
from jax.experimental.pallas import tpu as pltpu
from jax.sharding import PartitionSpec as P

MESH = pl.DeviceIdType.MESH
BF16 = jnp.bfloat16
F32 = jnp.float32
RING = 4
CHUNKS = 4
HALF = 128 // CHUNKS
ROWS = 8 * HALF
STEP = 16
COLS = 512
WIDE = 1024
N_REMOTE = 160
N_LOCAL = 32


class Place:
    def __init__(self, ssem, rsem, lsem):
        d = lax.axis_index('data')
        self.c = c = lax.axis_index('stage')
        self.z = z = d // 16
        self.y = y = (d // 4) % 4
        self.x = x = d % 4
        self.ssem, self.rsem, self.lsem = ssem, rsem, lsem
        self.n_slots = self.n_local = 0
        self.a1, self.a2 = self.order(y, x, c)
        self.z_ring = (z, self.dev((z + 1) % 4, y, x, c), self.dev((z + 3) % 4, y, x, c))
        k = 1 - c
        self.ring1 = (self.a1, self.dev(z, (y + c) % 4, (x + k) % 4, c), self.dev(z, (y + 3 * c) % 4, (x + 3 * k) % 4, c))
        self.ring2 = (self.a2, self.dev(z, (y + k) % 4, (x + c) % 4, c), self.dev(z, (y + 3 * k) % 4, (x + 3 * c) % 4, c))
        self.partner = self.dev(z, y, x, 1 - c)

    @staticmethod
    def order(y, x, c):
        return (1 - c) * x + c * y, (1 - c) * y + c * x

    @staticmethod
    def dev(z, y, x, c):
        return (z * 16 + y * 4 + x, c)

    def slots(self, n):
        self.n_slots += n
        assert self.n_slots <= N_REMOTE
        return self.n_slots - n

    def local_slots(self, n):
        self.n_local += n
        assert self.n_local <= N_LOCAL
        return self.n_local - n

    def local(self, src, dst, slot):
        return pltpu.make_async_copy(src, dst, self.lsem.at[slot])

    def remote(self, src, dst, dev, slot):
        return pltpu.make_async_remote_copy(src_ref=src, dst_ref=dst, send_sem=self.ssem.at[slot], recv_sem=self.rsem.at[slot], device_id=dev, device_id_type=MESH)

    def barrier(self):
        sem = pltpu.get_barrier_semaphore()
        z, y, x, c = self.z, self.y, self.x, self.c
        peers = [self.partner]
        for dz in range(1, 4):
            peers.append(self.dev((z + dz) % 4, y, x, c))
            peers.append(self.dev((z + dz) % 4, y, x, 1 - c))
        peers += [self.ring1[1], self.ring1[2], self.ring2[1], self.ring2[2]]
        for peer in peers:
            pl.semaphore_signal(sem, inc=1, device_id=peer, device_id_type=MESH)
        pl.semaphore_wait(sem, len(peers))


class Gather:
    def __init__(self, place, ring, at, base):
        self.pl, self.at, self.base = place, at, base
        self.me, self.plus, self.minus = ring

    def copy(self, i):
        me = self.me
        before, after = (me + 3) % 4, (me + 1) % 4
        j, h, dev = (
            (me, 0, self.plus), (me, 1, self.minus), (me, 1, self.plus), (me, 0, self.minus), (before, 0, self.plus), (after, 1, self.minus),
        )[i]
        return self.pl.remote(self.at(j, h), self.at(j, h), dev, self.base + i)

    def start(self):
        for i in range(4):
            self.copy(i).start()

    def relay(self):
        for i in range(2):
            self.copy(i).wait_recv()
            self.copy(4 + i).start()

    def near(self):
        self.copy(2).wait_recv()
        self.copy(3).wait_recv()

    def far(self):
        self.copy(4).wait_recv()
        self.copy(5).wait_recv()
        for i in range(6):
            self.copy(i).wait_send()

    def finish(self):
        self.near()
        self.far()


class Reduce:
    def __init__(self, place, ring, own, held, add, base):
        self.pl, self.own, self.held, self.add, self.base = place, own, held, add, base
        self.me, self.plus, self.minus = ring

    def copy(self, i):
        me, own, held = self.me, self.own, self.held
        far, after, before = (me + 2) % 4, (me + 1) % 4, (me + 3) % 4
        if i == 0:
            src, dst = own(far, 0), held(0).at[0]
        elif i == 1:
            src, dst = own(far, 1), held(0).at[1]
        elif i == 2:
            src, dst = own(after, 1), held(1).at[1]
        elif i == 3:
            src, dst = own(before, 0), held(2).at[0]
        elif i == 4:
            src, dst = held(0).at[0], held(1).at[0]
        else:
            src, dst = held(0).at[1], held(2).at[1]
        return self.pl.remote(src, dst, self.minus if i % 2 else self.plus, self.base + i)

    def start(self):
        for i in range(4):
            self.copy(i).start()

    def relay(self):
        for i in range(2):
            self.copy(i).wait_recv()
            self.add(i, (self.me + 3) % 4 if i else (self.me + 1) % 4)
            self.copy(4 + i).start()

    def finish(self):
        for i in range(2, 6):
            self.copy(i).wait_recv()
        for i in range(6):
            self.copy(i).wait_send()


def loop(n, body, start=0):
    def one(i, carry):
        body(i)
        return carry
    lax.fori_loop(start, n, one, 0)


def by_rows(body):
    def one(i):
        body(i // (HALF // STEP), pl.ds(pl.multiple_of(i % (HALF // STEP) * STEP, STEP), STEP))
    loop(2 * HALF // STEP, one)


def inverse_rms(rows):
    return lax.rsqrt(jnp.mean(rows * rows, axis=-1, keepdims=True) + 1e-6)


def rms(rows):
    return (rows * inverse_rms(rows)).astype(BF16)


def cotangent(h, e, dn):
    r = inverse_rms(h)
    back = r * dn - h * (r * r * r * jnp.mean(h * dn, axis=-1, keepdims=True))
    return (e + back).astype(BF16)


class Rows:
    def __init__(self, place, part, held):
        self.pl, self.part, self.held = place, part, held
        self.base = place.slots(6 * CHUNKS)

    def __call__(self, k):
        part, held = self.part, self.held

        def add(h, j):
            def one(i):
                rows = pl.ds(pl.multiple_of(i * STEP, STEP), STEP)
                held[0, k, h, rows] = held[0, k, h, rows] + part[k, j, h, rows]
            loop(HALF // STEP, one)
        return Reduce(self.pl, self.pl.z_ring, lambda j, h: part.at[k, j, h], lambda b: held.at[b, k], add, self.base + 6 * k)

    def total(self, k, h, rows):
        return self.part[k, self.pl.z, h, rows] + self.held[1, k, h, rows] + self.held[2, k, h, rows]


class Spreads:
    def __init__(self, place, ref):
        self.pl, self.ref = place, ref
        self.base = place.slots(6 * CHUNKS)

    def __call__(self, k):
        return Gather(self.pl, self.pl.z_ring, lambda j, h: self.ref.at[k, j, h], self.base + 6 * k)


class Weights:
    def __init__(self, place, s, shards, held, outs):
        self.pl, self.s, self.shards, self.held, self.outs = place, s, shards, held, outs
        self.slots = place.slots(8)
        self.out_slot = place.slots(1)
        self.swap_slots = place.slots(3)
        self.local = place.local_slots(3)
        self.copy_local = place.local_slots(3)
        self.first = Gather(place, place.ring2, lambda j, h: held.at[place.a1, j, h], place.slots(6))
        self.second = Gather(place, place.ring1, lambda j, h: held.at[j, 2 * h:2 * h + 2], place.slots(6))

    def parts(self, dz):
        place = self.pl
        target = (place.z + dz) % 4
        core = place.z // 2
        a1, a2 = place.order(place.y, place.x, core)
        cols = pl.ds(pl.multiple_of(target * WIDE, WIDE), WIDE)
        for m in range(2):
            yield m, self.shards[m].at[:, cols], self.held.at[a1, a2, place.z % 2, m], place.dev(target, place.y, place.x, core)

    def out_part(self, core):
        a1, a2 = self.pl.order(self.pl.y, self.pl.x, core)
        return self.shards[2].at[2 * core:2 * core + 2], self.held.at[a1, a2, :, 2]

    def source(self, act_remote, act_local):
        place, s = self.pl, self.s
        mine = place.z // 2 == s

        @pl.when(place.c == s)
        def _():
            for dz in range(1, 4):
                for m, src, dst, dev in self.parts(dz):
                    act_remote(place.remote(src, dst, dev, self.slots + 2 * dz + m))

            @pl.when(mine)
            def _():
                for m, src, dst, _ in self.parts(0):
                    act_local(place.local(src, dst, self.local + m))

            @pl.when(jnp.logical_not(mine))
            def _():
                for m, src, dst, _ in self.parts(0):
                    act_remote(place.remote(src, dst, place.partner, self.slots + m))
            src, dst = self.out_part(s)
            act_local(place.local(src, dst, self.local + 2))
            src, dst = self.out_part(1 - s)
            act_remote(place.remote(src, dst, place.partner, self.out_slot))

    def send(self):
        self.source(lambda copy: copy.start(), lambda copy: copy.start())

    def arrive(self):
        place, s = self.pl, self.s
        for dz in range(4):
            source = (place.z + 4 - dz) % 4
            here = source // 2 == place.c
            if dz == 0:
                here = jnp.logical_and(here, place.c != s)

            @pl.when(here)
            def _(dz=dz, source=source):
                for m in range(2):
                    dst = self.held.at[place.a1, place.a2, source % 2, m]
                    place.remote(dst, dst, place.partner, self.slots + 2 * dz + m).wait_recv()

        self.source(lambda copy: copy.wait_send(), lambda copy: copy.wait())

        @pl.when(place.c != s)
        def _():
            _, dst = self.out_part(1 - s)
            place.remote(dst, dst, place.partner, self.out_slot).wait_recv()

    def place_of(self, m, p, core):
        if m < 2:
            return self.outs[m].at[pl.ds(2 * core, 2), p]
        return self.outs[m].at[p, pl.ds(2 * core, 2)]

    def half_of(self, m, core):
        if m < 2:
            return self.outs[m].at[pl.ds(2 * core, 2)]
        return self.outs[m].at[:, pl.ds(2 * core, 2)]

    def spread(self, a1):
        place = self.pl

        def one(a2):
            x, y = place.order(a2, a1, place.c)
            p = y * 4 + x
            for m in range(3):
                src = self.held.at[a1, a2, :, m]
                dst = self.place_of(m, p, place.c)
                place.remote(src, dst, place.partner, self.swap_slots + m).start()
                place.local(src, dst, self.copy_local + m).start()
        loop(4, one)

    def done(self):
        place = self.pl
        for m in range(3):
            mine, other = self.half_of(m, place.c), self.half_of(m, 1 - place.c)
            place.remote(mine, other, place.partner, self.swap_slots + m).wait_recv()
            place.remote(mine, other, place.partner, self.swap_slots + m).wait_send()
            place.local(mine, mine, self.copy_local + m).wait()

    def step1(self):
        self.arrive()
        self.first.start()

    def step2(self):
        self.first.relay()

    def step3(self):
        self.first.finish()
        self.second.start()
        self.spread(self.pl.a1)

    def step4(self):
        self.second.relay()

    def step5(self):
        self.second.near()
        self.spread((self.pl.a1 + 3) % 4)
        self.spread((self.pl.a1 + 1) % 4)

    def step6(self):
        self.second.far()
        self.spread((self.pl.a1 + 2) % 4)


class Grads:
    def __init__(self, place, s, m, part, bufs, out):
        self.pl, self.s, self.m, self.part, self.out = place, s, m, part, out
        mine, held1, sum1, held2, sum2 = (buf.at[m] for buf in bufs)
        self.mine, self.held1, self.sum1, self.held2, self.sum2 = mine, held1, sum1, held2, sum2
        self.swap_slot = place.slots(1)
        self.hand_slots = place.slots(4)
        self.local = place.local_slots(1)

        def add1(h, j):
            def one(i):
                k, q = i // 2, i % 2
                held1[0, h, k, q] = held1[0, h, k, q] + mine[j, 2 * h + k, q]
            loop(4, one)
        self.first = Reduce(place, place.ring1, lambda j, h: mine.at[j, 2 * h:2 * h + 2], lambda b: held1.at[b], add1, place.slots(6))

        def add2(h, j):
            held2[0, h] = held2[0, h] + sum1[j, h]
        self.second = Reduce(place, place.ring2, lambda j, h: sum1.at[j, h], lambda b: held2.at[b], add2, place.slots(6))

    def part_of(self, p, core):
        if self.m < 2:
            return self.part.at[pl.ds(2 * core, 2), p]
        return self.part.at[p, pl.ds(2 * core, 2)]

    def swap(self):
        place = self.pl

        def one(p):
            other = 1 - place.c
            a1, a2 = place.order(p // 4, p % 4, other)
            place.remote(self.part_of(p, other), self.mine.at[a1, a2], place.partner, self.swap_slot).start()
        loop(16, one)

    def combine(self):
        place, mine = self.pl, self.mine
        whole = place.remote(mine, mine, place.partner, self.swap_slot)
        whole.wait_recv()

        def one(p):
            a1, a2 = place.order(p // 4, p % 4, place.c)
            for q in range(2):
                own = self.part[2 * place.c + q, p] if self.m < 2 else self.part[p, 2 * place.c + q]
                mine[a1, a2, q] = mine[a1, a2, q] + own
        loop(16, one)
        self.first.start()
        whole.wait_send()

    def turn(self):
        place, mine, held1, sum1 = self.pl, self.mine, self.held1, self.sum1
        self.first.finish()

        def one(i):
            h, k, q = i // 4, i // 2 % 2, i % 2
            sum1[i // 2, q] = mine[place.a1, i // 2, q] + held1[1, h, k, q] + held1[2, h, k, q]
        loop(8, one)
        self.second.start()

    def last(self):
        place = self.pl
        self.second.finish()
        for h in range(2):
            self.sum2[h] = self.sum1[place.a2, h] + self.held2[1, h] + self.held2[2, h]
        self.hand(False)

    def shard(self, source):
        return self.out.at[:, pl.ds(pl.multiple_of(source * WIDE, WIDE), WIDE)]

    def hand(self, wait):
        place, s = self.pl, self.s
        to_self = place.c == s

        def stay(src, dst):
            copy = place.local(src, dst, self.local)
            copy.wait() if wait else copy.start()

        def go(src, dst, dev, slot):
            copy = place.remote(src, dst, dev, slot)
            copy.wait_send() if wait else copy.start()

        if self.m == 2:
            rows = self.out.at[pl.ds(2 * place.c, 2)]
            pl.when(to_self)(lambda: stay(self.sum2, rows))
            pl.when(jnp.logical_not(to_self))(lambda: go(self.sum2, rows, place.partner, self.hand_slots))
            return
        for dz in range(4):
            target = (place.z + dz) % 4
            src, dst = self.sum2.at[target % 2], self.shard(place.z)
            here = target // 2 == place.c
            send = functools.partial(go, src, dst, place.dev(target, place.y, place.x, s), self.hand_slots + dz)
            if dz:
                pl.when(here)(send)
            else:
                pl.when(jnp.logical_and(here, to_self))(functools.partial(stay, src, dst))
                pl.when(jnp.logical_and(here, jnp.logical_not(to_self)))(send)

    def done(self):
        place, s = self.pl, self.s

        def land(dst, slot):
            place.remote(dst, dst, place.partner, slot).wait_recv()

        @pl.when(place.c == s)
        def _():
            if self.m == 2:
                land(self.out.at[pl.ds(2 * (1 - place.c), 2)], self.hand_slots)
                return
            for dz in range(1, 4):
                land(self.shard((place.z + 4 - dz) % 4), self.hand_slots + dz)
            pl.when(place.z // 2 != s)(lambda: land(self.shard(place.z), self.hand_slots))
        self.hand(True)


def mm(a, b):
    return jnp.dot(a, b, preferred_element_type=F32)


def mm_nt(a, b):
    return lax.dot_general(a, b, (((1,), (1,)), ((), ())), preferred_element_type=F32)


def mm_tn(a, b):
    return lax.dot_general(a, b, (((0,), (0,)), ((), ())), preferred_element_type=F32)


def at_cols(i):
    return pl.ds(pl.multiple_of(i * COLS, COLS), COLS)


def chunk(ref, k):
    return ref[k].reshape(ROWS, WIDE)


def pre_acts(n_ref, k, gate, inn, a_ref, b_ref, slot):
    def one(i):
        cols = at_cols(i)
        n = chunk(n_ref, k)
        a_ref[slot, :, cols] = mm(n, gate[:, :, :, cols].reshape(WIDE, COLS))
        b_ref[slot, :, cols] = mm(n, inn[:, :, :, cols].reshape(WIDE, COLS))
    loop(WIDE // COLS, one)


def hidden(a_ref, b_ref, slot, u_ref, k):
    def one(i):
        rows = pl.ds(pl.multiple_of(i * STEP, STEP), STEP)
        a = a_ref[slot, rows]
        u_ref[k, rows] = (a * jax.nn.sigmoid(a) * b_ref[slot, rows]).astype(BF16)
    loop(ROWS // STEP, one)


def project(u_ref, k, out, part):
    def one(i):
        cols = at_cols(i)
        o = mm(u_ref[k], out[:, :, :, cols].reshape(WIDE, COLS))
        part[k, :, :, :, cols] = o.reshape(4, 2, HALF, COLS)
    loop(WIDE // COLS, one)


def hidden_back(e_ref, k, out, t_ref, a_ref, b_ref, slot, da_ref, db_ref):
    def dot(i):
        t_ref[:, at_cols(i)] = mm_nt(chunk(e_ref, k), out[pl.ds(8 * i, 8)].reshape(COLS, WIDE))
    loop(WIDE // COLS, dot)

    def one(i):
        rows = pl.ds(pl.multiple_of(i * STEP, STEP), STEP)
        t, a, b = t_ref[rows], a_ref[slot, rows], b_ref[slot, rows]
        s = jax.nn.sigmoid(a)
        da_ref[k, rows] = (t * b * s * (1.0 + a * (1.0 - s))).astype(BF16)
        db_ref[k, rows] = (t * a * s).astype(BF16)
    loop(ROWS // STEP, one)


def input_back(da_ref, db_ref, k, gate, inn, part):
    def one(i):
        dn = mm_nt(da_ref[k], gate[pl.ds(2 * i, 2)].reshape(COLS, WIDE)) + mm_nt(db_ref[k], inn[pl.ds(2 * i, 2)].reshape(COLS, WIDE))
        part[k, :, :, :, at_cols(i)] = dn.reshape(4, 2, HALF, COLS)
    loop(WIDE // COLS, one)


def weight_grad(lhs, rhs, out, m):
    def one(i):
        cols = pl.ds(pl.multiple_of(i * 256, 256), 256)
        left = lhs[..., cols].reshape(CHUNKS * ROWS, 256)
        d = mm_tn(left, rhs[...].reshape(CHUNKS * ROWS, WIDE))
        if m < 2:
            out[i] = d.reshape(16, 16, WIDE)
        else:
            out[pl.ds(4 * i, 4)] = d.reshape(4, 4, 16, WIDE)
    loop(4, one)


def kernel_1(x_ref, g_ref, wg, wi, wo, ga_ref, h_ref, n1_ref, n0_out, a_out, b_out, u_out, v1g, v1i, v1o,
             n0, a_s, b_s, u_s, part, held, w0g, w0i, w0o, held_w, held_w1, ssem, rsem, lsem):
    place = Place(ssem, rsem, lsem)
    z, c = place.z, place.c
    shards = (wg, wi, wo)
    w0 = Weights(place, 0, shards, held_w, (w0g, w0i, w0o))
    w1 = Weights(place, 1, shards, held_w1, (v1g, v1i, v1o))
    rows_n0, rows_g, rows_o, rows_n1 = Spreads(place, n0), Spreads(place, ga_ref), Rows(place, part, held), Spreads(place, n1_ref)
    g_copy = place.local(g_ref.at[c], ga_ref.at[:, z], place.local_slots(1))
    save = place.local_slots(4)

    def saves(k):
        return (
            place.local(a_s.at[k], a_out.at[k], save + 0), place.local(b_s.at[k], b_out.at[k], save + 1), place.local(u_s.at[k], u_out.at[k], save + 2),
        )
    n0_save = place.local(n0, n0_out, save + 3)

    place.barrier()
    w0.send()
    g_copy.start()

    def start_n0(k):
        def norm(h, rows):
            n0[k, z, h, rows] = rms(x_ref[c, k, h, rows].astype(F32))
        by_rows(norm)
        rows_n0(k).start()
    loop(CHUNKS, start_n0)
    w0.step1()
    rows_n0(0).relay()
    w0.step2()
    loop(CHUNKS, lambda k: rows_n0(k).relay(), 1)
    w0.step3()
    g_copy.wait()
    loop(CHUNKS, lambda k: rows_n0(k).finish())
    n0_save.start()
    loop(CHUNKS, lambda k: rows_g(k).start())
    w0.step4()
    w1.send()
    w0.step5()
    loop(CHUNKS, lambda k: rows_g(k).relay())
    w0.step6()
    w1.step1()
    w0.done()

    def pipeline(i):
        @pl.when(i < CHUNKS)
        def _():
            @pl.when(i >= 1)
            def _():
                for copy in saves(i - 1):
                    copy.wait()
            pre_acts(n0, i, w0g, w0i, a_s, b_s, i)
            hidden(a_s, b_s, i, u_s, i)
            for copy in saves(i):
                copy.start()
            project(u_s, i, w0o, part)
            rows_o(i).start()
        pl.when(jnp.logical_and(i >= 1, i <= CHUNKS))(lambda: rows_o(i - 1).relay())
        pl.when(i == 0)(lambda: w1.step2())
        pl.when(i == 1)(lambda: w1.step3())
        pl.when(i == 2)(lambda: w1.step4())
        pl.when(i == 3)(lambda: w1.step5())
        pl.when(i == 4)(lambda: w1.step6())

        @pl.when(jnp.logical_and(i >= 2, i <= CHUNKS + 1))
        def _():
            k = i - 2
            rows_o(k).finish()

            def step(h, rows):
                o = rows_o.total(k, h, rows).astype(BF16).astype(F32)
                out = (x_ref[c, k, h, rows].astype(F32) + o).astype(BF16)
                h_ref[k, h, rows] = out
                n1_ref[k, z, h, rows] = rms(out.astype(F32))
            by_rows(step)
            rows_n1(k).start()
        pl.when(i >= 3)(lambda: rows_n1(i - 3).relay())
    loop(CHUNKS + 3, pipeline)
    for copy in saves(CHUNKS - 1):
        copy.wait()
    n0_save.wait()
    loop(CHUNKS, lambda k: rows_g(k).finish())
    w1.done()
    loop(CHUNKS, lambda k: rows_n1(k).finish())


def three_grads(place, s, parts, bufs, outs):
    return [Grads(place, s, m, parts[m], bufs, outs[m]) for m in range(3)]


def kernel_2(n1, ga, h_ref, v1g, v1i, v1o, wg, wi, wo, e_ref, eo_ref, v0g, v0i, v0o, gg, gi, go,
             w1g, w1i, w1o, a_s, b_s, t_s, u_s, da_s, db_s, part, held, held_w, dg, di, do, mine, held1, sum1, held2, sum2, ssem, rsem, lsem):
    place = Place(ssem, rsem, lsem)
    z = place.z
    load = place.local_slots(3)
    loads = [place.local(v, w, load + m) for m, (v, w) in enumerate(((v1g, w1g), (v1i, w1i), (v1o, w1o)))]
    for copy in loads:
        copy.start()
    w0 = Weights(place, 0, (wg, wi, wo), held_w, (v0g, v0i, v0o))
    rows_d, rows_e = Rows(place, part, held), Spreads(place, e_ref)
    gate, inn, out = three_grads(place, 1, (dg, di, do), (mine, held1, sum1, held2, sum2), (gg, gi, go))
    place.barrier()
    w0.send()
    for copy in loads:
        copy.wait()

    def ahead(k):
        pre_acts(n1, k, w1g, w1i, a_s, b_s, k % 2)
        hidden(a_s, b_s, k % 2, u_s, k)

    def back(k):
        hidden_back(ga, k, w1o, t_s, a_s, b_s, k % 2, da_s, db_s)
        input_back(da_s, db_s, k, w1g, w1i, part)
        rows_d(k).start()

    def close(k):
        rows_d(k).finish()

        def step(h, rows):
            dn = rows_d.total(k, h, rows)
            e = cotangent(h_ref[k, h, rows].astype(F32), ga[k, z, h, rows].astype(F32), dn)
            e_ref[k, z, h, rows] = e
            eo_ref[k, h, rows] = e
        by_rows(step)
        rows_e(k).start()

    def early(k):
        ahead(k)
        back(k)
        pl.when(k == 0)(w0.step1)
        pl.when(k == 1)(w0.step2)
    loop(2, early)
    rows_d(0).relay()
    w0.step3()

    def middle(k):
        ahead(k)
        pl.when(k == 2)(w0.step4)
    loop(4, middle, 2)
    rows_d(1).relay()
    weight_grad(u_s, ga, do, 2)
    out.swap()
    w0.step5()

    def late(k):
        back(k)
        close(k - 2)
        pl.when(k == 2)(w0.step6)
    loop(4, late, 2)
    out.combine()
    rows_d(2).relay()
    weight_grad(n1, da_s, dg, 0)
    gate.swap()
    rows_d(3).relay()
    rows_e(0).relay()
    rows_e(1).relay()
    weight_grad(n1, db_s, di, 1)
    inn.swap()
    close(2)
    out.first.relay()
    gate.combine()
    close(3)
    inn.combine()
    rows_e(2).relay()
    out.turn()
    gate.first.relay()
    rows_e(3).relay()
    out.second.relay()
    inn.first.relay()
    out.last()
    gate.turn()
    w0.done()
    gate.second.relay()
    inn.turn()
    gate.last()
    inn.second.relay()
    loop(CHUNKS, lambda k: rows_e(k).finish())
    inn.last()
    out.done()
    gate.done()
    inn.done()


def kernel_3(e_ref, x_ref, eo_ref, n0_in, a_in, b_in, u_in, v0g, v0i, v0o, dx_ref, gg, gi, go,
             w0g, w0i, w0o, n0, a_s, b_s, t_s, u_s, da_s, db_s, part, held, dg, di, do, mine, held1, sum1, held2, sum2, ssem, rsem, lsem):
    place = Place(ssem, rsem, lsem)
    c = place.c
    load = place.local_slots(5)
    loads = [place.local(v, w, load + m) for m, (v, w) in enumerate(((v0o, w0o), (v0g, w0g), (v0i, w0i), (u_in, u_s), (n0_in, n0)))]
    load_ab = place.local_slots(4)

    def loads_ab(k):
        return place.local(a_in.at[k], a_s.at[k % 2], load_ab + 2 * (k % 2)), place.local(b_in.at[k], b_s.at[k % 2], load_ab + 2 * (k % 2) + 1)
    loads[0].start()
    for copy in loads_ab(0):
        copy.start()
    loads[1].start()
    loads[2].start()
    for copy in loads_ab(1):
        copy.start()
    loads[3].start()
    loads[4].start()
    rows_d = Rows(place, part, held)
    gate, inn, out = three_grads(place, 0, (dg, di, do), (mine, held1, sum1, held2, sum2), (gg, gi, go))
    swap = place.remote(dx_ref.at[c], dx_ref.at[c], place.partner, place.slots(1))
    place.barrier()
    for copy in loads[:3]:
        copy.wait()

    def hide(k):
        for copy in loads_ab(k):
            copy.wait()
        hidden_back(e_ref, k, w0o, t_s, a_s, b_s, k % 2, da_s, db_s)

    def close(k):
        rows_d(k).finish()

        def step(h, rows):
            dn = rows_d.total(k, h, rows)
            dx_ref[c, k, h, rows] = cotangent(x_ref[c, k, h, rows].astype(F32), eo_ref[k, h, rows].astype(F32), dn)
        by_rows(step)

    def early(k):
        hide(k)
        for copy in loads_ab(k + 2):
            copy.start()
        input_back(da_s, db_s, k, w0g, w0i, part)
        rows_d(k).start()
    loop(2, early)
    loads[3].wait()
    weight_grad(u_s, e_ref, do, 2)
    out.swap()
    rows_d(0).relay()
    loop(4, hide, 2)
    loads[4].wait()
    out.combine()
    rows_d(1).relay()
    weight_grad(n0, da_s, dg, 0)
    gate.swap()

    def late(k):
        input_back(da_s, db_s, k, w0g, w0i, part)
        rows_d(k).start()
        close(k - 2)
    loop(4, late, 2)
    gate.combine()
    weight_grad(n0, db_s, di, 1)
    inn.swap()
    rows_d(2).relay()
    out.first.relay()
    rows_d(3).relay()
    inn.combine()
    gate.first.relay()
    out.turn()
    close(2)
    inn.first.relay()
    out.second.relay()
    gate.turn()
    out.last()
    close(3)
    swap.start()
    gate.second.relay()
    inn.turn()
    gate.last()
    inn.second.relay()
    inn.last()
    swap.wait()
    out.done()
    gate.done()
    inn.done()


VM = pl.BlockSpec(memory_space=pltpu.VMEM)
ANY = pl.BlockSpec(memory_space=pl.ANY)


def sds(shape, dtype):
    return jax.ShapeDtypeStruct(shape, dtype)


ALL_ROWS = (CHUNKS, 4, 2, HALF, WIDE)
OWN_ROWS = (CHUNKS, 2, HALF, WIDE)
FLAT_ROWS = (CHUNKS, ROWS, WIDE)
UP = (4, 16, 16, WIDE)
DOWN = (16, 4, 16, WIDE)
W_SHAPES = [sds(UP, BF16), sds(UP, BF16), sds(DOWN, BF16)]
G_SHAPES = [sds((16, 4 * WIDE), F32), sds((16, 4 * WIDE), F32), sds((4, 16, WIDE), F32)]
ROW_BUFS = [pltpu.VMEM(ALL_ROWS, F32), pltpu.VMEM((3,) + OWN_ROWS, F32)]
W_FULL = [pltpu.VMEM(UP, BF16), pltpu.VMEM(UP, BF16), pltpu.VMEM(DOWN, BF16)]
W_HELD = pltpu.VMEM((4, 4, 2, 3, 16, WIDE), BF16)
BACK_BUFS = [pltpu.VMEM((2, ROWS, WIDE), F32)] * 2 + [pltpu.VMEM((ROWS, WIDE), F32)] + [pltpu.VMEM(FLAT_ROWS, BF16)] * 3
G_BUFS = [
    pltpu.VMEM(UP, F32),
    pltpu.VMEM(UP, F32),
    pltpu.VMEM(DOWN, F32),
    pltpu.VMEM((3, 4, 4, 2, 16, WIDE), F32),
    pltpu.VMEM((3, 3, 2, 2, 2, 16, WIDE), F32),
    pltpu.VMEM((3, 4, 2, 16, WIDE), F32),
    pltpu.VMEM((3, 3, 2, 16, WIDE), F32),
    pltpu.VMEM((3, 2, 16, WIDE), F32),
]
SEMS = [pltpu.SemaphoreType.DMA((N_REMOTE,)), pltpu.SemaphoreType.DMA((N_REMOTE,)), pltpu.SemaphoreType.DMA((N_LOCAL,))]


def call(kernel, cid, ins, outs, out_specs, scratch):
    return pl.pallas_call(
        kernel,
        out_shape=outs,
        in_specs=ins,
        out_specs=out_specs,
        scratch_shapes=scratch + SEMS,
        compiler_params=pltpu.CompilerParams(collective_id=cid, has_side_effects=True, vmem_limit_bytes=67043328),
        name=kernel.__name__,
    )


def solution(mesh):
    act_spec = P(None, 'data', None, None)
    weight_spec = P('stage', None, 'data', None)

    def per_device(x, g, w_gate, w_in, w_out):
        xs = x.reshape((2,) + OWN_ROWS)
        gs = g.reshape((2,) + OWN_ROWS)
        shards = (w_gate.reshape(16, 4 * WIDE), w_in.reshape(16, 4 * WIDE), w_out.reshape(4, 16, WIDE))

        outs = [sds(ALL_ROWS, BF16), sds(OWN_ROWS, BF16), sds(ALL_ROWS, BF16)]
        outs += [sds(ALL_ROWS, BF16), sds(FLAT_ROWS, F32), sds(FLAT_ROWS, F32), sds(FLAT_ROWS, BF16)] + W_SHAPES
        scratch = [pltpu.VMEM(ALL_ROWS, BF16), pltpu.VMEM(FLAT_ROWS, F32), pltpu.VMEM(FLAT_ROWS, F32), pltpu.VMEM(FLAT_ROWS, BF16)]
        scratch += ROW_BUFS + W_FULL + [W_HELD] * 2
        g_all, h1, n1, n0, a0, b0, u0, *w1 = call(kernel_1, 1, [VM] * 5, outs, [VM] * 3 + [ANY] * 7, scratch)(xs, gs, *shards)

        outs = [sds(ALL_ROWS, BF16), sds(OWN_ROWS, BF16)] + W_SHAPES + G_SHAPES
        scratch = W_FULL + BACK_BUFS + ROW_BUFS + [W_HELD] + G_BUFS
        e_all, e_own, *rest = call(kernel_2, 2, [VM] * 3 + [ANY] * 3 + [VM] * 3, outs, [VM] * 2 + [ANY] * 3 + [VM] * 3, scratch)(n1, g_all, h1, *w1, *shards)
        w0, own1 = rest[:3], rest[3:]

        outs = [sds((2,) + OWN_ROWS, BF16)] + G_SHAPES
        scratch = W_FULL + [pltpu.VMEM(ALL_ROWS, BF16)] + BACK_BUFS + ROW_BUFS + G_BUFS
        dx, *own0 = call(kernel_3, 3, [VM] * 3 + [ANY] * 7, outs, [VM] * 4, scratch)(e_all, xs, e_own, n0, a0, b0, u0, *w0)
        first = lax.axis_index('stage') == 0
        own = [jnp.where(first, s0, s1) for s0, s1 in zip(own0, own1)]
        return (dx.reshape(x.shape), own[0].reshape(w_gate.shape), own[1].reshape(w_in.shape), own[2].reshape(w_out.shape))

    return jax.shard_map(per_device, mesh=mesh, in_specs=(act_spec, act_spec, weight_spec, weight_spec, weight_spec), out_specs=(act_spec, weight_spec, weight_spec, weight_spec), check_vma=False)
```

```python
import functools

import jax
import jax.numpy as jnp
from jax import lax
from jax.experimental import pallas as pl
from jax.experimental.pallas import tpu as pltpu
from jax.sharding import PartitionSpec as P

MESH = pl.DeviceIdType.MESH
BF16 = jnp.bfloat16
F32 = jnp.float32
RING = 4
CHUNKS = 4
HALF = 128 // CHUNKS
ROWS = 8 * HALF
STEP = 16
COLS = 512
WIDE = 1024
N_REMOTE = 224
N_LOCAL = 40


class Place:
    def __init__(self, ssem, rsem, lsem, phase):
        d = lax.axis_index('data')
        self.c = lax.axis_index('stage')
        self.z, self.y, self.x = d // 16, (d // 4) % 4, d % 4
        self.ssem, self.rsem, self.lsem, self.phase = ssem, rsem, lsem, phase
        self.n_slots = self.n_local = 0
        self.partner = self.dev(self.z, self.y, self.x, 1 - self.c)

    @staticmethod
    def dev(z, y, x, c):
        return (z * 16 + y * 4 + x, c)

    def slots(self, n):
        self.n_slots += n
        assert self.n_slots <= N_REMOTE
        return self.n_slots - n

    def local_slots(self, n):
        self.n_local += n
        assert self.n_local <= N_LOCAL
        return self.n_local - n

    def local(self, src, dst, slot):
        return pltpu.make_async_copy(src, dst, self.lsem.at[slot])

    def remote(self, src, dst, dev, slot):
        return pltpu.make_async_remote_copy(src_ref=src, dst_ref=dst, send_sem=self.ssem.at[slot], recv_sem=self.rsem.at[slot], device_id=dev, device_id_type=MESH)

    def peers(self):
        z, y, x, c = self.z, self.y, self.x, self.c
        peers = [self.partner, self.dev(z, y, (x + 1) % 4, c), self.dev(z, y, (x + 3) % 4, c)]
        for step in range(1, 4):
            for core in (c, 1 - c):
                peers.append(self.dev((z + step) % 4, y, x, core))
                peers.append(self.dev(z, (y + step) % 4, x, core))
        return peers

    def signal(self, sem):
        for peer in self.peers():
            pl.semaphore_signal(sem, inc=1, device_id=peer, device_id_type=MESH)

    def wait(self, sem):
        pl.semaphore_wait(sem, len(self.peers()))


class Block:
    def __init__(self, place, b):
        self.b, self.c, self.x = b, place.c, place.x
        self.t, self.w = (place.z, place.y) if b == 0 else (place.y, place.z)
        t, w, x, c, k = self.t, self.w, self.x, self.c, 1 - self.c
        self.a1, self.a2 = self.order(w, x, c)
        self.rows = (t, self.dev((t + 1) % 4, w, x, c), self.dev((t + 3) % 4, w, x, c))
        self.ring1 = (self.a1, self.dev(t, (w + c) % 4, (x + k) % 4, c), self.dev(t, (w + 3 * c) % 4, (x + 3 * k) % 4, c))
        self.ring2 = (self.a2, self.dev(t, (w + k) % 4, (x + c) % 4, c), self.dev(t, (w + 3 * k) % 4, (x + 3 * c) % 4, c))

    def dev(self, t, w, x, c):
        return Place.dev(t, w, x, c) if self.b == 0 else Place.dev(w, t, x, c)

    @staticmethod
    def order(w, x, c):
        return (1 - c) * x + c * w, (1 - c) * w + c * x

    def index(self, m, w, x, q):
        return (w, x, q) if m == 2 else (q, w, x) if self.b == 0 else (w, q, x)

    def pieces(self, position):
        if self.b == 0:
            return [(pl.ds(pl.multiple_of(position * WIDE, WIDE), WIDE), pl.ds(0, WIDE))]
        return [(pl.ds(pl.multiple_of(u * WIDE + position * 256, 256), 256), pl.ds(u * 256, 256)) for u in range(4)]


def pair(core):
    return pl.ds(2 * core, 2)


class Gather:
    def __init__(self, place, ring, at, base):
        self.pl, self.at, self.base = place, at, base
        self.me, self.plus, self.minus = ring

    def copy(self, i):
        me = self.me
        before, after = (me + 3) % 4, (me + 1) % 4
        j, h, dev = (
            (me, 0, self.plus), (me, 1, self.minus), (me, 1, self.plus), (me, 0, self.minus), (before, 0, self.plus), (after, 1, self.minus),
        )[i]
        return self.pl.remote(self.at(j, h), self.at(j, h), dev, self.base + i)

    def start(self):
        for i in range(4):
            self.copy(i).start()

    def relay(self):
        for i in range(2):
            self.copy(i).wait_recv()
            self.copy(4 + i).start()

    def near(self):
        self.copy(2).wait_recv()
        self.copy(3).wait_recv()

    def far(self):
        self.copy(4).wait_recv()
        self.copy(5).wait_recv()
        for i in range(6):
            self.copy(i).wait_send()

    def finish(self):
        self.near()
        self.far()


class Reduce:
    def __init__(self, place, ring, own, held, add, base):
        self.pl, self.own, self.held, self.add, self.base = place, own, held, add, base
        self.me, self.plus, self.minus = ring

    def copy(self, i):
        me, own, held = self.me, self.own, self.held
        far, after, before = (me + 2) % 4, (me + 1) % 4, (me + 3) % 4
        if i == 0:
            src, dst = own(far, 0), held(0).at[0]
        elif i == 1:
            src, dst = own(far, 1), held(0).at[1]
        elif i == 2:
            src, dst = own(after, 1), held(1).at[1]
        elif i == 3:
            src, dst = own(before, 0), held(2).at[0]
        elif i == 4:
            src, dst = held(0).at[0], held(1).at[0]
        else:
            src, dst = held(0).at[1], held(2).at[1]
        return self.pl.remote(src, dst, self.minus if i % 2 else self.plus, self.base + i)

    def start(self):
        for i in range(4):
            self.copy(i).start()

    def relay(self):
        for i in range(2):
            self.copy(i).wait_recv()
            self.add(i, (self.me + 3) % 4 if i else (self.me + 1) % 4)
            self.copy(4 + i).start()

    def finish(self):
        for i in range(2, 6):
            self.copy(i).wait_recv()
        for i in range(6):
            self.copy(i).wait_send()


def loop(n, body, start=0):
    def one(i, carry):
        body(i)
        return carry
    lax.fori_loop(start, n, one, 0)


def by_rows(body):
    def one(i):
        body(i // (HALF // STEP), pl.ds(pl.multiple_of(i % (HALF // STEP) * STEP, STEP), STEP))
    loop(2 * HALF // STEP, one)


def inverse_rms(rows):
    return lax.rsqrt(jnp.mean(rows * rows, axis=-1, keepdims=True) + 1e-6)


def rms(rows):
    return (rows * inverse_rms(rows)).astype(BF16)


def cotangent(h, e, dn):
    r = inverse_rms(h)
    back = r * dn - h * (r * r * r * jnp.mean(h * dn, axis=-1, keepdims=True))
    return (e + back).astype(BF16)


class Rows:
    def __init__(self, place, ring, part, held, base):
        self.pl, self.ring, self.part, self.held, self.base = place, ring, part, held, base

    def __call__(self, k):
        part, held = self.part, self.held

        def add(h, j):
            def one(i):
                rows = pl.ds(pl.multiple_of(i * STEP, STEP), STEP)
                held[0, k, h, rows] = held[0, k, h, rows] + part[k, j, h, rows]
            loop(HALF // STEP, one)
        return Reduce(self.pl, self.ring, lambda j, h: part.at[k, j, h], lambda b: held.at[b, k], add, self.base + 6 * k)

    def total(self, k, h, rows):
        return self.part[k, self.ring[0], h, rows] + self.held[1, k, h, rows] + self.held[2, k, h, rows]


class Spreads:
    def __init__(self, place, ring, ref, base):
        self.pl, self.ring, self.ref, self.base = place, ring, ref, base

    def __call__(self, k):
        return Gather(self.pl, self.ring, lambda j, h: self.ref.at[k, j, h], self.base + 6 * k)


class Weights:
    def __init__(self, place, block, shards, held, outs, base, local):
        self.pl, self.bk, self.s, self.shards, self.held, self.outs = place, block, block.b, shards, held, outs
        self.slots, self.out_slot, self.swap_slots = base, base + 8, base + 9
        self.local, self.copy_local = local, local + 3
        self.first = Gather(place, block.ring2, lambda j, h: held.at[block.a1, j, h], base + 12)
        self.second = Gather(place, block.ring1, lambda j, h: held.at[j, 2 * h:2 * h + 2], base + 18)

    def parts(self, dz):
        bk = self.bk
        target = (bk.t + dz) % 4
        core = bk.t // 2
        a1, a2 = bk.order(bk.w, bk.x, core)
        for m in range(2):
            whole = self.held.at[a1, a2, bk.t % 2, m]
            copies = [(self.shards[m].at[:, src], self.held.at[a1, a2, bk.t % 2, m, :, dst]) for src, dst in bk.pieces(target)]
            yield m, copies, whole, bk.dev(target, bk.w, bk.x, core)

    def out_part(self, core):
        a1, a2 = self.bk.order(self.bk.w, self.bk.x, core)
        return self.shards[2].at[2 * core:2 * core + 2], self.held.at[a1, a2, :, 2]

    def source(self, wait):
        place, s = self.pl, self.s
        mine = self.bk.t // 2 == s

        def away(copies, whole, dev, slot):
            if wait:
                place.remote(whole, whole, dev, slot).wait_send()
                return
            for src, dst in copies:
                place.remote(src, dst, dev, slot).start()

        def here(copies, whole, slot):
            if wait:
                place.local(whole, whole, slot).wait()
                return
            for src, dst in copies:
                place.local(src, dst, slot).start()

        @pl.when(place.c == s)
        def _():
            for dz in range(1, 4):
                for m, copies, whole, dev in self.parts(dz):
                    away(copies, whole, dev, self.slots + 2 * dz + m)

            @pl.when(mine)
            def _():
                for m, copies, whole, _ in self.parts(0):
                    here(copies, whole, self.local + m)

            @pl.when(jnp.logical_not(mine))
            def _():
                for m, copies, whole, _ in self.parts(0):
                    away(copies, whole, place.partner, self.slots + m)
            src, dst = self.out_part(s)
            here([(src, dst)], dst, self.local + 2)
            src, dst = self.out_part(1 - s)
            away([(src, dst)], dst, place.partner, self.out_slot)

    def send(self):
        self.source(False)

    def arrive(self):
        place, bk, s = self.pl, self.bk, self.s
        for dz in range(4):
            source = (bk.t + 4 - dz) % 4
            here = source // 2 == place.c
            if dz == 0:
                here = jnp.logical_and(here, place.c != s)

            @pl.when(here)
            def _(dz=dz, source=source):
                for m in range(2):
                    dst = self.held.at[bk.a1, bk.a2, source % 2, m]
                    place.remote(dst, dst, place.partner, self.slots + 2 * dz + m).wait_recv()

        self.source(True)

        @pl.when(place.c != s)
        def _():
            _, dst = self.out_part(1 - s)
            place.remote(dst, dst, place.partner, self.out_slot).wait_recv()

    def spread(self, a1):
        place, bk = self.pl, self.bk

        def one(a2):
            x, w = bk.order(a2, a1, place.c)
            for m in range(3):
                src = self.held.at[a1, a2, :, m]
                dst = self.outs[m].at[bk.index(m, w, x, pair(place.c))]
                place.remote(src, dst, place.partner, self.swap_slots + m).start()
                place.local(src, dst, self.copy_local + m).start()
        loop(4, one)

    def done(self):
        place, bk = self.pl, self.bk
        every = slice(None)
        for m in range(3):
            mine, other = (self.outs[m].at[bk.index(m, every, every, pair(core))] for core in (place.c, 1 - place.c))
            place.remote(mine, other, place.partner, self.swap_slots + m).wait_recv()
            place.remote(mine, other, place.partner, self.swap_slots + m).wait_send()
            place.local(mine, mine, self.copy_local + m).wait()

    def step1(self):
        self.arrive()
        self.first.start()

    def step2(self):
        self.first.relay()

    def step3(self):
        self.first.finish()
        self.second.start()
        self.spread(self.bk.a1)

    def step4(self):
        self.second.relay()

    def step5(self):
        self.second.near()
        self.spread((self.bk.a1 + 3) % 4)
        self.spread((self.bk.a1 + 1) % 4)

    def step6(self):
        self.second.far()
        self.spread((self.bk.a1 + 2) % 4)


class Grads:
    def __init__(self, place, block, m, part, bufs, out, base, local):
        self.pl, self.bk, self.s, self.m, self.part, self.out = place, block, block.b, m, part, out
        mine, held1, sum1, held2, sum2 = (buf.at[m] for buf in bufs)
        self.mine, self.held1, self.sum1, self.held2, self.sum2 = mine, held1, sum1, held2, sum2
        base, self.local = base + 17 * m, local + m
        self.swap_slot, self.hand_slots = base, base + 1

        def add1(h, j):
            def one(i):
                k, q = i // 2, i % 2
                held1[0, h, k, q] = held1[0, h, k, q] + mine[j, 2 * h + k, q]
            loop(4, one)
        self.first = Reduce(place, block.ring1, lambda j, h: mine.at[j, 2 * h:2 * h + 2], lambda b: held1.at[b], add1, base + 5)

        def add2(h, j):
            held2[0, h] = held2[0, h] + sum1[j, h]
        self.second = Reduce(place, block.ring2, lambda j, h: sum1.at[j, h], lambda b: held2.at[b], add2, base + 11)

    def swap(self):
        place, bk = self.pl, self.bk

        def one(p):
            w, x, other = p // 4, p % 4, 1 - place.c
            a1, a2 = bk.order(w, x, other)
            src = self.part.at[bk.index(self.m, w, x, pair(other))]
            place.remote(src, self.mine.at[a1, a2], place.partner, self.swap_slot).start()
        loop(16, one)

    def combine(self):
        place, bk, mine = self.pl, self.bk, self.mine
        whole = place.remote(mine, mine, place.partner, self.swap_slot)
        whole.wait_recv()

        def one(p):
            w, x = p // 4, p % 4
            a1, a2 = bk.order(w, x, place.c)
            for q in range(2):
                mine[a1, a2, q] = mine[a1, a2, q] + self.part[bk.index(self.m, w, x, 2 * place.c + q)]
        loop(16, one)
        self.first.start()
        whole.wait_send()

    def turn(self):
        bk, mine, held1, sum1 = self.bk, self.mine, self.held1, self.sum1
        self.first.finish()

        def one(i):
            h, k, q = i // 4, i // 2 % 2, i % 2
            sum1[i // 2, q] = mine[bk.a1, i // 2, q] + held1[1, h, k, q] + held1[2, h, k, q]
        loop(8, one)
        self.second.start()

    def last(self):
        self.second.finish()
        for h in range(2):
            self.sum2[h] = self.sum1[self.bk.a2, h] + self.held2[1, h] + self.held2[2, h]
        self.hand(False)

    def hand(self, wait):
        place, bk, s = self.pl, self.bk, self.s
        to_self = place.c == s

        def stay(copies, whole):
            if wait:
                place.local(whole, whole, self.local).wait()
                return
            for src, dst in copies:
                place.local(src, dst, self.local).start()

        def go(copies, whole, dev, slot):
            if wait:
                place.remote(whole, whole, dev, slot).wait_send()
                return
            for src, dst in copies:
                place.remote(src, dst, dev, slot).start()

        if self.m == 2:
            copies = [(self.sum2, self.out.at[pair(place.c)])]
            pl.when(to_self)(lambda: stay(copies, self.sum2))
            pl.when(jnp.logical_not(to_self))(lambda: go(copies, self.sum2, place.partner, self.hand_slots))
            return
        for dz in range(4):
            target = (bk.t + dz) % 4
            whole = self.sum2.at[target % 2]
            copies = [(self.sum2.at[target % 2, :, own], self.out.at[:, shard]) for shard, own in bk.pieces(bk.t)]
            here = target // 2 == place.c
            send = functools.partial(go, copies, whole, bk.dev(target, bk.w, bk.x, s), self.hand_slots + dz)
            if dz:
                pl.when(here)(send)
            else:
                pl.when(jnp.logical_and(here, to_self))(functools.partial(stay, copies, whole))
                pl.when(jnp.logical_and(here, jnp.logical_not(to_self)))(send)

    def done(self):
        place, bk, s = self.pl, self.bk, self.s

        def land(like, slot):
            place.remote(like, like, place.partner, slot).wait_recv()

        @pl.when(place.c == s)
        def _():
            if self.m == 2:
                land(self.sum2, self.hand_slots)
                return
            for dz in range(1, 4):
                land(self.sum2.at[0], self.hand_slots + dz)
            pl.when(bk.t // 2 != s)(lambda: land(self.sum2.at[0], self.hand_slots))
        self.hand(True)


def mm(a, b):
    return jnp.dot(a, b, preferred_element_type=F32)


def mm_nt(a, b):
    return lax.dot_general(a, b, (((1,), (1,)), ((), ())), preferred_element_type=F32)


def mm_tn(a, b):
    return lax.dot_general(a, b, (((0,), (0,)), ((), ())), preferred_element_type=F32)


def chunk(ref, k):
    return ref[k].reshape(ROWS, WIDE)


def square(ref):
    return ref[...].reshape(WIDE, WIDE)


def pre_acts(n_ref, k, gate, inn, a_ref, b_ref, slot):
    a_ref[slot] = mm(chunk(n_ref, k), square(gate))
    b_ref[slot] = mm(chunk(n_ref, k), square(inn))


def hidden(a_ref, b_ref, slot, u_ref, k):
    def one(i):
        rows = pl.ds(pl.multiple_of(i * STEP, STEP), STEP)
        a = a_ref[slot, rows]
        u_ref[k, rows] = (a * jax.nn.sigmoid(a) * b_ref[slot, rows]).astype(BF16)
    loop(ROWS // STEP, one)


def project(u_ref, k, out, part):
    part[k] = mm(u_ref[k], square(out)).reshape(4, 2, HALF, WIDE)


def hidden_back(e_ref, k, out, t_ref, a_ref, b_ref, slot, da_ref, db_ref):
    t_ref[k] = mm_nt(chunk(e_ref, k), square(out)).reshape(4, 2, HALF, WIDE)
    per_half = HALF // STEP

    def one(i):
        rows = pl.ds(pl.multiple_of(i * STEP, STEP), STEP)
        j = i // (2 * per_half)
        h = i // per_half % 2
        t = t_ref[k, j, h, pl.ds(pl.multiple_of(i % per_half * STEP, STEP), STEP)]
        a, b = a_ref[slot, rows], b_ref[slot, rows]
        s = jax.nn.sigmoid(a)
        da_ref[k, rows] = (t * b * s * (1.0 + a * (1.0 - s))).astype(BF16)
        db_ref[k, rows] = (t * a * s).astype(BF16)
    loop(ROWS // STEP, one)


def input_back(da_ref, db_ref, k, gate, inn, part):
    def one(i):
        cols = pl.ds(pl.multiple_of(i * COLS, COLS), COLS)
        dn = mm_nt(da_ref[k], gate[pl.ds(2 * i, 2)].reshape(COLS, WIDE)) + mm_nt(db_ref[k], inn[pl.ds(2 * i, 2)].reshape(COLS, WIDE))
        part[k, :, :, :, cols] = dn.reshape(4, 2, HALF, COLS)
    loop(WIDE // COLS, one)


def weight_grad(lhs, rhs, out):
    def one(i):
        cols = pl.ds(pl.multiple_of(i * 256, 256), 256)
        left = lhs[..., cols].reshape(CHUNKS * ROWS, 256)
        out[i] = mm_tn(left, rhs[...].reshape(CHUNKS * ROWS, WIDE)).reshape(4, 4, 16, WIDE)
    loop(4, one)


def kernel(x_in, g_in, wg, wi, wo, dx_out, gg, gi, go, a_out, b_out, u_out, n_out,
           xs, hs, dxs, n0e, n1, ga, u_s, a_s, b_s, da_s, db_s, part, held, w0g, w0i, w0o, w1g, w1i, w1o, held_w,
           d_a, d_b, mine, held1, sum1, held2, sum2, ssem, rsem, lsem, phase):
    place = Place(ssem, rsem, lsem, phase)
    z, y, c = place.z, place.y, place.c
    blocks = Block(place, 0), Block(place, 1)
    per_row = 6 * CHUNKS
    z_gather, z_sum, g_gather, y_gather, y_sum = (place.slots(per_row) for _ in range(5))
    rows_n0, rows_e = (Spreads(place, blocks[0].rows, n0e, z_gather) for _ in range(2))
    rows_o, rows_d0 = (Rows(place, blocks[0].rows, part, held, z_sum) for _ in range(2))
    rows_g = Spreads(place, blocks[1].rows, ga, g_gather)
    rows_n1 = Spreads(place, blocks[1].rows, n1, y_gather)
    rows_d1 = Rows(place, blocks[1].rows, part, held, y_sum)
    shards = (wg, wi, wo)
    w0_slots, w0_local = place.slots(24), place.local_slots(6)
    w0, w0b = (Weights(place, blocks[0], shards, held_w, (w0g, w0i, w0o), w0_slots, w0_local) for _ in range(2))
    w1 = Weights(place, blocks[1], shards, held_w, (w1g, w1i, w1o), place.slots(24), place.local_slots(6))
    grad_slots, grad_local = place.slots(51), place.local_slots(3)
    bufs, outs = (mine, held1, sum1, held2, sum2), (gg, gi, go)
    (gate1, inn1, out1), (gate0, inn0, out0) = (
        [Grads(place, blocks[b], m, (d_b, d_a, d_a)[m], bufs, outs[m], grad_slots, grad_local) for m in range(3)] for b in (1, 0)
    )
    x_copy = place.local(x_in.at[c], xs, place.local_slots(1))
    g_copy = place.local(g_in.at[c], ga.at[:, y], place.local_slots(1))
    save = place.local_slots(8)
    n_save, n_load = place.local(n0e, n_out, save + 6), place.local(n_out, n1, save + 6)
    u_load = place.local(u_out, u_s, save + 7)

    def saves(k):
        slot = k % 2
        at = save + 3 * slot
        return place.local(a_s.at[slot], a_out.at[k], at), place.local(b_s.at[slot], b_out.at[k], at + 1), place.local(u_s.at[k], u_out.at[k], at + 2)

    def loads(k):
        slot = k % 2
        at = save + 3 * slot
        return place.local(a_out.at[k], a_s.at[slot], at), place.local(b_out.at[k], b_s.at[slot], at + 1)

    def start(copies):
        for copy in copies:
            copy.start()

    def wait(copies):
        for copy in copies:
            copy.wait()

    def at(condition, *steps):
        @pl.when(condition)
        def _():
            for step in steps:
                step()

    x_copy.start()
    g_copy.start()
    barrier = pltpu.get_barrier_semaphore()
    place.signal(barrier)
    place.wait(barrier)
    w0.send()
    x_copy.wait()

    def start_n0(k):
        def norm(h, rows):
            n0e[k, z, h, rows] = rms(xs[k, h, rows].astype(F32))
        by_rows(norm)
        rows_n0(k).start()
    loop(CHUNKS, start_n0)
    w0.step1()
    rows_n0(0).relay()
    w0.step2()
    loop(CHUNKS, lambda k: rows_n0(k).relay(), 1)
    w0.step3()
    w0.step4()
    loop(CHUNKS, lambda k: rows_n0(k).finish())
    n_save.start()
    g_copy.wait()
    w0.step5()
    w0.step6()
    loop(CHUNKS, lambda k: rows_g(k).start())
    w0.done()
    place.signal(phase.at[0])

    def close_o(k):
        rows_o(k).finish()

        def step(h, rows):
            o = rows_o.total(k, h, rows).astype(BF16).astype(F32)
            out = (xs[k, h, rows].astype(F32) + o).astype(BF16)
            hs[k, h, rows] = out
            n1[k, y, h, rows] = rms(out.astype(F32))
        by_rows(step)
        rows_n1(k).start()

    def forward(i):
        at(i >= 2, lambda: wait(saves(i - 2)))
        pre_acts(n0e, i, w0g, w0i, a_s, b_s, i % 2)
        at(i == 0, lambda: place.wait(phase.at[0]), w1.send)
        at(i == 1, w1.step2)
        at(i == 2, w1.step4)
        at(i == 3, w1.step5, rows_n1(0).relay)
        hidden(a_s, b_s, i % 2, u_s, i)
        start(saves(i))
        project(u_s, i, w0o, part)
        rows_o(i).start()
        at(i >= 1, lambda: rows_o(i - 1).relay())
        at(i == 0, w1.step1, lambda: loop(CHUNKS, lambda k: rows_g(k).relay()))
        at(i == 1, w1.step3)
        at(i >= 2, lambda: close_o(i - 2))
        at(i == 3, w1.step6)
    loop(CHUNKS, forward)
    rows_o(3).relay()
    wait(saves(2))
    wait(saves(3))
    n_save.wait()
    loop(CHUNKS, lambda k: rows_g(k).finish())
    w1.done()
    place.signal(phase.at[1])

    def close_1(k):
        rows_d1(k).finish()

        def step(h, rows):
            dn = rows_d1.total(k, h, rows)
            n0e[k, z, h, rows] = cotangent(hs[k, h, rows].astype(F32), ga[k, y, h, rows].astype(F32), dn)
        by_rows(step)
        rows_e(k).start()

    def middle(j):
        rows_n1(j).finish()
        pre_acts(n1, j, w1g, w1i, a_s, b_s, j % 2)
        hidden(a_s, b_s, j % 2, u_s, j)
        at(j <= 2, lambda: rows_n1(j + 1).relay())
        at(j <= 1, lambda: close_o(j + 2))
        at(j >= 1, lambda: rows_d1(j - 1).relay())
        at(j == 1, lambda: place.wait(phase.at[1]), w0b.send)
        at(j == 2, w0b.step1)
        at(j == 3, w0b.step3, rows_e(0).relay)
        hidden_back(ga, j, w1o, part, a_s, b_s, j % 2, da_s, db_s)
        input_back(da_s, db_s, j, w1g, w1i, part)
        rows_d1(j).start()
        at(j == 2, w0b.step2)
        at(j == 3, w0b.step4)
        at(j >= 2, lambda: start(loads(j - 2)), lambda: close_1(j - 2))
    loop(CHUNKS, middle)
    rows_d1(3).relay()
    weight_grad(u_s, ga, d_a)
    out1.swap()
    u_load.start()
    rows_e(1).relay()
    w0b.step5()
    weight_grad(n1, da_s, d_b)
    gate1.swap()
    close_1(2)
    w0b.step6()
    out1.combine()
    weight_grad(n1, db_s, d_a)
    inn1.swap()
    n_load.start()
    close_1(3)
    rows_e(2).relay()
    out1.first.relay()
    gate1.combine()
    w0b.done()

    def close_0(k):
        rows_d0(k).finish()

        def step(h, rows):
            dn = rows_d0.total(k, h, rows)
            dxs[k, h, rows] = cotangent(xs[k, h, rows].astype(F32), n0e[k, z, h, rows].astype(F32), dn)
        by_rows(step)

    def backward(i):
        rows_e(i).finish()
        wait(loads(i))
        hidden_back(n0e, i, w0o, part, a_s, b_s, i % 2, da_s, db_s)
        at(i <= 1, lambda: start(loads(i + 2)))
        at(i == 0, rows_e(3).relay, inn1.combine, gate1.first.relay)
        at(i == 1, inn1.first.relay, gate1.turn, out1.second.relay)
        at(i == 2, inn1.second.relay, gate1.last)
        at(i == 3, out1.done, gate1.done, inn1.done, lambda: place.signal(phase.at[2]))
        input_back(da_s, db_s, i, w0g, w0i, part)
        rows_d0(i).start()
        at(i >= 1, lambda: rows_d0(i - 1).relay())
        at(i == 0, out1.turn)
        at(i == 1, inn1.turn, gate1.second.relay, out1.last)
        at(i == 2, inn1.last)
        at(i >= 2, lambda: close_0(i - 2))
    loop(CHUNKS, backward)
    u_load.wait()
    weight_grad(u_s, n0e, d_a)
    place.wait(phase.at[2])
    out0.swap()
    rows_d0(3).relay()
    n_load.wait()
    weight_grad(n1, da_s, d_b)
    gate0.swap()
    close_0(2)
    out0.combine()
    weight_grad(n1, db_s, d_a)
    inn0.swap()
    out0.first.relay()
    gate0.combine()
    close_0(3)
    dx_slot, dx_local = place.slots(1), place.local_slots(1)
    dx_away, dx_here = place.remote(dxs, dx_out.at[c], place.partner, dx_slot), place.local(dxs, dx_out.at[c], dx_local)
    dx_away.start()
    dx_here.start()
    inn0.combine()
    gate0.first.relay()
    out0.turn()
    inn0.first.relay()
    out0.second.relay()
    gate0.turn()
    out0.last()
    inn0.turn()
    gate0.second.relay()
    gate0.last()
    inn0.second.relay()
    inn0.last()
    dx_away.wait()
    dx_here.wait()
    out0.done()
    gate0.done()
    inn0.done()


VM = pl.BlockSpec(memory_space=pltpu.VMEM)
ANY = pl.BlockSpec(memory_space=pl.ANY)


def sds(shape, dtype):
    return jax.ShapeDtypeStruct(shape, dtype)


ALL_ROWS = (CHUNKS, 4, 2, HALF, WIDE)
OWN_ROWS = (CHUNKS, 2, HALF, WIDE)
FLAT_ROWS = (CHUNKS, ROWS, WIDE)
WEIGHT = (4, 4, 4, 16, WIDE)
OUTS = [
    sds((2,) + OWN_ROWS, BF16), sds((16, 4 * WIDE), F32), sds((16, 4 * WIDE), F32), sds((4, 16, WIDE), F32),
    sds(FLAT_ROWS, F32), sds(FLAT_ROWS, F32), sds(FLAT_ROWS, BF16), sds(ALL_ROWS, BF16),
]
SCRATCH = (
    [pltpu.VMEM(OWN_ROWS, BF16)] * 3
    + [pltpu.VMEM(ALL_ROWS, BF16)] * 3
    + [pltpu.VMEM(FLAT_ROWS, BF16)]
    + [pltpu.VMEM((2, ROWS, WIDE), F32)] * 2
    + [pltpu.VMEM(FLAT_ROWS, BF16)] * 2
    + [pltpu.VMEM(ALL_ROWS, F32), pltpu.VMEM((3,) + OWN_ROWS, F32)]
    + [pltpu.VMEM(WEIGHT, BF16)] * 6
    + [pltpu.VMEM((4, 4, 2, 3, 16, WIDE), BF16)]
    + [pltpu.VMEM(WEIGHT, F32)] * 2
    + [
        pltpu.VMEM((3, 4, 4, 2, 16, WIDE), F32),
        pltpu.VMEM((3, 3, 2, 2, 2, 16, WIDE), F32),
        pltpu.VMEM((3, 4, 2, 16, WIDE), F32),
        pltpu.VMEM((3, 3, 2, 16, WIDE), F32),
        pltpu.VMEM((3, 2, 16, WIDE), F32),
    ]
    + [pltpu.SemaphoreType.DMA((N_REMOTE,)), pltpu.SemaphoreType.DMA((N_REMOTE,)), pltpu.SemaphoreType.DMA((N_LOCAL,))]
    + [pltpu.SemaphoreType.REGULAR((3,))]
)


def call(*operands):
    return pl.pallas_call(
        kernel,
        out_shape=OUTS,
        in_specs=[ANY] * 2 + [VM] * 3,
        out_specs=[ANY] * len(OUTS),
        scratch_shapes=SCRATCH,
        compiler_params=pltpu.CompilerParams(collective_id=1, has_side_effects=True, vmem_limit_bytes=67043328),
        name='kernel_all',
    )(*operands)


def solution(mesh):
    act_spec = P(None, 'data', None, None)
    weight_spec = P('stage', None, 'data', None)

    def per_device(x, g, w_gate, w_in, w_out):
        shards = (w_gate.reshape(16, 4 * WIDE), w_in.reshape(16, 4 * WIDE), w_out.reshape(4, 16, WIDE))
        dx, d_gate, d_in, d_out, *_ = call(x.reshape((2,) + OWN_ROWS), g.reshape((2,) + OWN_ROWS), *shards)
        return dx.reshape(x.shape), d_gate.reshape(w_gate.shape), d_in.reshape(w_in.shape), d_out.reshape(w_out.shape)

    return jax.shard_map(per_device, mesh=mesh, in_specs=(act_spec, act_spec, weight_spec, weight_spec, weight_spec), out_specs=(act_spec, weight_spec, weight_spec, weight_spec), check_vma=False)
```

```python
import functools

import jax
import jax.numpy as jnp
from jax import lax
from jax.experimental import pallas as pl
from jax.experimental.pallas import tpu as pltpu
from jax.sharding import PartitionSpec as P

MESH = pl.DeviceIdType.MESH
BF16 = jnp.bfloat16
F32 = jnp.float32
RING = 4
CHUNKS = 4
HALF = 128 // CHUNKS
ROWS = 8 * HALF
STEP = 16
GROUPS = ROWS // STEP
COLS = 512
WIDE = 1024
N_REMOTE = 280
N_LOCAL = 40


class Place:
    def __init__(self, ssem, rsem, lsem, phase):
        d = lax.axis_index('data')
        self.c = lax.axis_index('stage')
        self.z, self.y, self.x = d // 16, (d // 4) % 4, d % 4
        self.ssem, self.rsem, self.lsem, self.phase = ssem, rsem, lsem, phase
        self.n_slots = self.n_local = 0
        self.partner = self.dev(self.z, self.y, self.x, 1 - self.c)

    @staticmethod
    def dev(z, y, x, c):
        return (z * 16 + y * 4 + x, c)

    def slots(self, n):
        self.n_slots += n
        assert self.n_slots <= N_REMOTE
        return self.n_slots - n

    def local_slots(self, n):
        self.n_local += n
        assert self.n_local <= N_LOCAL
        return self.n_local - n

    def local(self, src, dst, slot):
        return pltpu.make_async_copy(src, dst, self.lsem.at[slot])

    def remote(self, src, dst, dev, slot):
        return pltpu.make_async_remote_copy(src_ref=src, dst_ref=dst, send_sem=self.ssem.at[slot], recv_sem=self.rsem.at[slot], device_id=dev, device_id_type=MESH)

    def peers(self):
        z, y, x, c = self.z, self.y, self.x, self.c
        peers = [self.partner, self.dev(z, y, (x + 1) % 4, c), self.dev(z, y, (x + 3) % 4, c)]
        for step in range(1, 4):
            for core in (c, 1 - c):
                peers.append(self.dev((z + step) % 4, y, x, core))
                peers.append(self.dev(z, (y + step) % 4, x, core))
        return peers

    def signal(self, sem):
        for peer in self.peers():
            pl.semaphore_signal(sem, inc=1, device_id=peer, device_id_type=MESH)

    def wait(self, sem):
        pl.semaphore_wait(sem, len(self.peers()))


class Block:
    def __init__(self, place, b, heavy):
        self.b, self.c, self.x = b, place.c, place.x
        self.t, self.w = (place.z, place.y) if b == 0 else (place.y, place.z)
        self.heavy = heavy
        t, w, x, c = self.t, self.w, self.x, self.c
        self.a1, self.a2 = self.order(w, x, c)
        self.rows = (t, self.dev((t + 1) % 4, w, x, c), self.dev((t + 3) % 4, w, x, c))
        v = self.turned(c)
        k = 1 - v
        self.ring1 = (self.a1, self.dev(t, (w + v) % 4, (x + k) % 4, c), self.dev(t, (w + 3 * v) % 4, (x + 3 * k) % 4, c))
        self.ring2 = (self.a2, self.dev(t, (w + k) % 4, (x + v) % 4, c), self.dev(t, (w + 3 * k) % 4, (x + 3 * v) % 4, c))

    def dev(self, t, w, x, c):
        return Place.dev(t, w, x, c) if self.b == 0 else Place.dev(w, t, x, c)

    def turned(self, core):
        return core if self.heavy == 'split' else int(self.heavy == 'w')

    def order(self, w, x, core):
        v = self.turned(core)
        return (1 - v) * x + v * w, (1 - v) * w + v * x

    def place(self, a1, a2, core):
        v = self.turned(core)
        return (1 - v) * a2 + v * a1, (1 - v) * a1 + v * a2

    def index(self, m, w, x, q):
        return (w, x, q) if m == 2 else (q, w, x) if self.b == 0 else (w, q, x)

    def pieces(self, position):
        if self.b == 0:
            return [(pl.ds(pl.multiple_of(position * WIDE, WIDE), WIDE), pl.ds(0, WIDE))]
        return [(pl.ds(pl.multiple_of(u * WIDE + position * 256, 256), 256), pl.ds(u * 256, 256)) for u in range(4)]


def pair(core):
    return pl.ds(2 * core, 2)


class Gather:
    def __init__(self, place, ring, at, base):
        self.pl, self.at, self.base = place, at, base
        self.me, self.plus, self.minus = ring

    def copy(self, i):
        me = self.me
        before, after = (me + 3) % 4, (me + 1) % 4
        j, h, dev = (
            (me, 0, self.plus), (me, 1, self.minus), (me, 1, self.plus), (me, 0, self.minus), (before, 0, self.plus), (after, 1, self.minus),
        )[i]
        return self.pl.remote(self.at(j, h), self.at(j, h), dev, self.base + i)

    def start(self):
        for i in range(4):
            self.copy(i).start()

    def relay(self):
        for i in range(2):
            self.copy(i).wait_recv()
            self.copy(4 + i).start()

    def near(self):
        self.copy(2).wait_recv()
        self.copy(3).wait_recv()

    def far(self):
        self.copy(4).wait_recv()
        self.copy(5).wait_recv()
        for i in range(6):
            self.copy(i).wait_send()

    def finish(self):
        self.near()
        self.far()


class Reduce:
    def __init__(self, place, ring, own, held, add, base):
        self.pl, self.own, self.held, self.add, self.base = place, own, held, add, base
        self.me, self.plus, self.minus = ring

    def copy(self, i):
        me, own, held = self.me, self.own, self.held
        far, after, before = (me + 2) % 4, (me + 1) % 4, (me + 3) % 4
        if i == 0:
            src, dst = own(far, 0), held(0).at[0]
        elif i == 1:
            src, dst = own(far, 1), held(0).at[1]
        elif i == 2:
            src, dst = own(after, 1), held(1).at[1]
        elif i == 3:
            src, dst = own(before, 0), held(2).at[0]
        elif i == 4:
            src, dst = held(0).at[0], held(1).at[0]
        else:
            src, dst = held(0).at[1], held(2).at[1]
        return self.pl.remote(src, dst, self.minus if i % 2 else self.plus, self.base + i)

    def start(self):
        for i in range(4):
            self.copy(i).start()

    def relay(self):
        for i in range(2):
            self.copy(i).wait_recv()
            self.add(i, (self.me + 3) % 4 if i else (self.me + 1) % 4)
            self.copy(4 + i).start()

    def finish(self):
        for i in range(2, 6):
            self.copy(i).wait_recv()
        for i in range(6):
            self.copy(i).wait_send()


def loop(n, body, start=0):
    def one(i, carry):
        body(i)
        return carry
    lax.fori_loop(start, n, one, 0)


def by_rows(body):
    def one(i):
        body(i // (HALF // STEP), pl.ds(pl.multiple_of(i % (HALF // STEP) * STEP, STEP), STEP))
    loop(2 * HALF // STEP, one)


def inverse_rms(rows):
    return lax.rsqrt(jnp.mean(rows * rows, axis=-1, keepdims=True) + 1e-6)


def rms(rows):
    return (rows * inverse_rms(rows)).astype(BF16)


def cotangent(h, e, dn):
    r = inverse_rms(h)
    back = r * dn - h * (r * r * r * jnp.mean(h * dn, axis=-1, keepdims=True))
    return (e + back).astype(BF16)


class Rows:
    def __init__(self, place, ring, part, held, base):
        self.pl, self.ring, self.part, self.held, self.base = place, ring, part, held, base

    def __call__(self, k):
        part, held = self.part, self.held

        def add(h, j):
            def one(i):
                rows = pl.ds(pl.multiple_of(i * STEP, STEP), STEP)
                held[0, k, h, rows] = held[0, k, h, rows] + part[k, j, h, rows]
            loop(HALF // STEP, one)
        return Reduce(self.pl, self.ring, lambda j, h: part.at[k, j, h], lambda b: held.at[b, k], add, self.base + 6 * k)

    def total(self, k, h, rows):
        return self.part[k, self.ring[0], h, rows] + self.held[1, k, h, rows] + self.held[2, k, h, rows]


class Spreads:
    def __init__(self, place, ring, ref, base):
        self.pl, self.ring, self.ref, self.base = place, ring, ref, base

    def __call__(self, k):
        return Gather(self.pl, self.ring, lambda j, h: self.ref.at[k, j, h], self.base + 6 * k)


class Weights:
    def __init__(self, place, block, shards, held, outs, base, local):
        self.pl, self.bk, self.s, self.shards, self.held, self.outs = place, block, block.b, shards, held, outs
        self.slots, self.out_slot, self.swap_slots = base, base + 8, base + 9
        self.local, self.copy_local = local, local + 3
        self.first = Gather(place, block.ring2, lambda j, h: held.at[block.a1, pl.ds((2 * j + h) * 3, 3)], base + 12)
        self.second = Gather(place, block.ring1, lambda j, h: held.at[j, 12 * h:12 * h + 12], base + 18)

    def piece(self, a1, a2, q, m):
        return self.held.at[a1, (2 * a2 + q) * 3 + m]

    def parts(self, dz):
        bk = self.bk
        target = (bk.t + dz) % 4
        core = bk.t // 2
        a1, a2 = bk.order(bk.w, bk.x, core)
        for m in range(2):
            whole = self.piece(a1, a2, bk.t % 2, m)
            copies = [(self.shards[m].at[:, src], whole.at[:, dst]) for src, dst in bk.pieces(target)]
            yield m, copies, whole, bk.dev(target, bk.w, bk.x, core)

    def out_part(self, core):
        a1, a2 = self.bk.order(self.bk.w, self.bk.x, core)
        copies = [(self.shards[2].at[2 * core + q], self.piece(a1, a2, q, 2)) for q in range(2)]
        return copies, self.held.at[a1, pl.ds(0, 2)]

    def source(self, wait):
        place, s = self.pl, self.s
        mine = self.bk.t // 2 == s

        def away(copies, whole, dev, slot):
            if wait:
                place.remote(whole, whole, dev, slot).wait_send()
                return
            for src, dst in copies:
                place.remote(src, dst, dev, slot).start()

        def here(copies, whole, slot):
            if wait:
                place.local(whole, whole, slot).wait()
                return
            for src, dst in copies:
                place.local(src, dst, slot).start()

        @pl.when(place.c == s)
        def _():
            for dz in range(1, 4):
                for m, copies, whole, dev in self.parts(dz):
                    away(copies, whole, dev, self.slots + 2 * dz + m)

            @pl.when(mine)
            def _():
                for m, copies, whole, _ in self.parts(0):
                    here(copies, whole, self.local + m)

            @pl.when(jnp.logical_not(mine))
            def _():
                for m, copies, whole, _ in self.parts(0):
                    away(copies, whole, place.partner, self.slots + m)
            here(*self.out_part(s), self.local + 2)
            away(*self.out_part(1 - s), place.partner, self.out_slot)

    def send(self):
        self.source(False)

    def arrive(self):
        place, bk, s = self.pl, self.bk, self.s
        for dz in range(4):
            source = (bk.t + 4 - dz) % 4
            here = source // 2 == place.c
            if dz == 0:
                here = jnp.logical_and(here, place.c != s)

            @pl.when(here)
            def _(dz=dz, source=source):
                for m in range(2):
                    dst = self.piece(bk.a1, bk.a2, source % 2, m)
                    place.remote(dst, dst, place.partner, self.slots + 2 * dz + m).wait_recv()

        self.source(True)

        @pl.when(place.c != s)
        def _():
            _, whole = self.out_part(1 - s)
            place.remote(whole, whole, place.partner, self.out_slot).wait_recv()

    def spread(self, a1):
        place, bk = self.pl, self.bk

        def one(a2):
            w, x = bk.place(a1, a2, place.c)
            for m in range(3):
                for q in range(2):
                    src = self.piece(a1, a2, q, m)
                    dst = self.outs[m].at[bk.index(m, w, x, 2 * place.c + q)]
                    place.remote(src, dst, place.partner, self.swap_slots + m).start()
                    place.local(src, dst, self.copy_local + m).start()
        loop(4, one)

    def done(self):
        place, bk = self.pl, self.bk
        every = slice(None)
        for m in range(3):
            mine, other = (self.outs[m].at[bk.index(m, every, every, pair(core))] for core in (place.c, 1 - place.c))
            place.remote(mine, other, place.partner, self.swap_slots + m).wait_recv()
            place.remote(mine, other, place.partner, self.swap_slots + m).wait_send()
            place.local(mine, mine, self.copy_local + m).wait()

    def step1(self):
        self.arrive()
        self.first.start()

    def step2(self):
        self.first.relay()

    def step3(self):
        self.first.finish()
        self.second.start()
        self.spread(self.bk.a1)

    def step4(self):
        self.second.relay()

    def step5(self):
        self.second.near()
        self.spread((self.bk.a1 + 3) % 4)
        self.spread((self.bk.a1 + 1) % 4)

    def step6(self):
        self.second.far()
        self.spread((self.bk.a1 + 2) % 4)


class Grads:
    def __init__(self, place, block, m, part, bufs, kit, out, base, local):
        self.pl, self.bk, self.s, self.m, self.part, self.out = place, block, block.b, m, part, out
        mine, held1, held2, sum2 = (buf.at[kit] for buf in bufs)
        self.mine, self.held1, self.held2, self.sum2 = mine, held1, held2, sum2
        self.local = local
        self.swap_slot, self.hand_slots = base, base + 1

        def add1(h, j):
            def one(i):
                k, q = i // 2, i % 2
                held1[0, h, k, q] = held1[0, h, k, q] + mine[j, 2 * h + k, q]
            loop(4, one)
        self.first = Reduce(place, block.ring1, lambda j, h: mine.at[j, 2 * h:2 * h + 2], lambda b: held1.at[b], add1, base + 5)

        def add2(h, j):
            held2[0, h] = held2[0, h] + mine[block.a1, j, h]
        self.second = Reduce(place, block.ring2, lambda j, h: mine.at[block.a1, j, h], lambda b: held2.at[b], add2, base + 11)

    def swap(self):
        place, bk = self.pl, self.bk

        def one(p):
            w, x, other = p // 4, p % 4, 1 - place.c
            a1, a2 = bk.order(w, x, other)
            src = self.part.at[bk.index(self.m, w, x, pair(other))]
            place.remote(src, self.mine.at[a1, a2], place.partner, self.swap_slot).start()
        loop(16, one)

    def combine(self):
        place, bk, mine = self.pl, self.bk, self.mine
        whole = place.remote(mine, mine, place.partner, self.swap_slot)
        whole.wait_recv()

        def one(p):
            w, x = p // 4, p % 4
            a1, a2 = bk.order(w, x, place.c)
            for q in range(2):
                mine[a1, a2, q] = mine[a1, a2, q] + self.part[bk.index(self.m, w, x, 2 * place.c + q)]
        loop(16, one)
        whole.wait_send()

    def turn(self):
        bk, mine, held1 = self.bk, self.mine, self.held1
        self.first.finish()

        def one(i):
            h, k, q = i // 4, i // 2 % 2, i % 2
            mine[bk.a1, i // 2, q] = mine[bk.a1, i // 2, q] + held1[1, h, k, q] + held1[2, h, k, q]
        loop(8, one)
        self.second.start()

    def last(self):
        self.second.finish()
        for h in range(2):
            self.sum2[h] = self.mine[self.bk.a1, self.bk.a2, h] + self.held2[1, h] + self.held2[2, h]
        self.hand(False)

    def hand(self, wait):
        place, bk, s = self.pl, self.bk, self.s
        to_self = place.c == s

        def stay(copies, whole):
            if wait:
                place.local(whole, whole, self.local).wait()
                return
            for src, dst in copies:
                place.local(src, dst, self.local).start()

        def go(copies, whole, dev, slot):
            if wait:
                place.remote(whole, whole, dev, slot).wait_send()
                return
            for src, dst in copies:
                place.remote(src, dst, dev, slot).start()

        if self.m == 2:
            copies = [(self.sum2, self.out.at[pair(place.c)])]
            pl.when(to_self)(lambda: stay(copies, self.sum2))
            pl.when(jnp.logical_not(to_self))(lambda: go(copies, self.sum2, place.partner, self.hand_slots))
            return
        for dz in range(4):
            target = (bk.t + dz) % 4
            whole = self.sum2.at[target % 2]
            copies = [(self.sum2.at[target % 2, :, own], self.out.at[:, shard]) for shard, own in bk.pieces(bk.t)]
            here = target // 2 == place.c
            send = functools.partial(go, copies, whole, bk.dev(target, bk.w, bk.x, s), self.hand_slots + dz)
            if dz:
                pl.when(here)(send)
            else:
                pl.when(jnp.logical_and(here, to_self))(functools.partial(stay, copies, whole))
                pl.when(jnp.logical_and(here, jnp.logical_not(to_self)))(send)

    def done(self):
        place, bk, s = self.pl, self.bk, self.s

        def land(like, slot):
            place.remote(like, like, place.partner, slot).wait_recv()

        @pl.when(place.c == s)
        def _():
            if self.m == 2:
                land(self.sum2, self.hand_slots)
                return
            for dz in range(1, 4):
                land(self.sum2.at[0], self.hand_slots + dz)
            pl.when(bk.t // 2 != s)(lambda: land(self.sum2.at[0], self.hand_slots))
        self.hand(True)


def mm(a, b):
    return jnp.dot(a, b, preferred_element_type=F32)


def mm_nt(a, b):
    return lax.dot_general(a, b, (((1,), (1,)), ((), ())), preferred_element_type=F32)


def mm_tn(a, b):
    return lax.dot_general(a, b, (((0,), (0,)), ((), ())), preferred_element_type=F32)


def chunk(ref, k):
    return ref[k].reshape(ROWS, WIDE)


def square(ref):
    return ref[...].reshape(WIDE, WIDE)


def pre_acts(n_ref, k, gate, inn, a_ref, b_ref, slot):
    a_ref[slot] = mm(chunk(n_ref, k), square(gate))
    b_ref[slot] = mm(chunk(n_ref, k), square(inn))


def hidden(a_ref, b_ref, slot, u_ref, k):
    def one(i):
        rows = pl.ds(pl.multiple_of(i * STEP, STEP), STEP)
        a = a_ref[slot, rows]
        u_ref[k, rows] = (a * jax.nn.sigmoid(a) * b_ref[slot, rows]).astype(BF16)
    loop(ROWS // STEP, one)


def project(u_ref, k, out, part):
    part[k] = mm(u_ref[k], square(out)).reshape(4, 2, HALF, WIDE)


def hidden_back(e_ref, k, out, t_ref, a_ref, b_ref, slot, dab):
    t_ref[k] = mm_nt(chunk(e_ref, k), square(out)).reshape(4, 2, HALF, WIDE)
    per_half = HALF // STEP

    def one(i):
        rows = pl.ds(pl.multiple_of(i * STEP, STEP), STEP)
        j = i // (2 * per_half)
        h = i // per_half % 2
        t = t_ref[k, j, h, pl.ds(pl.multiple_of(i % per_half * STEP, STEP), STEP)]
        a, b = a_ref[slot, rows], b_ref[slot, rows]
        s = jax.nn.sigmoid(a)
        dab[k, i] = (t * b * s * (1.0 + a * (1.0 - s))).astype(BF16)
        dab[k, GROUPS + i] = (t * a * s).astype(BF16)
    loop(ROWS // STEP, one)


def input_back(dab, k, gate, inn, part):
    def one(i):
        da, db = dab[k, :GROUPS].reshape(ROWS, WIDE), dab[k, GROUPS:].reshape(ROWS, WIDE)
        cols = pl.ds(pl.multiple_of(i * COLS, COLS), COLS)
        dn = mm_nt(da, gate[pl.ds(2 * i, 2)].reshape(COLS, WIDE)) + mm_nt(db, inn[pl.ds(2 * i, 2)].reshape(COLS, WIDE))
        part[k, :, :, :, cols] = dn.reshape(4, 2, HALF, COLS)
    loop(WIDE // COLS, one)


def weight_grad(lhs, rhs, out):
    def one(i):
        cols = pl.ds(pl.multiple_of(i * 256, 256), 256)
        left = lhs[..., cols].reshape(CHUNKS * ROWS, 256)
        out[i] = mm_tn(left, rhs[...].reshape(CHUNKS * ROWS, WIDE)).reshape(4, 4, 16, WIDE)
    loop(4, one)


def weight_grad_of(n_ref, dab, first, out):
    def one(i):
        cols = pl.ds(pl.multiple_of(i * 256, 256), 256)
        right = dab[:, first:first + GROUPS].reshape(CHUNKS * ROWS, WIDE)
        out[i] = mm_tn(n_ref[..., cols].reshape(CHUNKS * ROWS, 256), right).reshape(4, 4, 16, WIDE)
    loop(4, one)


HEAVY = {'w0': 'split', 'w1': 'x', 'v0': 'x', 'out1': 'x', 'gate1': 'split', 'inn1': 'split', 'out0': 'split', 'gate0': 'split', 'inn0': 'split'}


def kernel(x_in, g_in, wg, wi, wo, dx_out, gg, gi, go, a_out, b_out, u_out, n_out, held_1, held_0,
           xs, hs, n0e, n1, ga, u_s, a_s, b_s, dab, part, held, w0g, w0i, w0o, w1g, w1i, w1o,
           d_a, d_b, mine, held1, held2, sum2, ssem, rsem, lsem, phase):
    place = Place(ssem, rsem, lsem, phase)
    z, y, c = place.z, place.y, place.c
    rows0, rows1 = Block(place, 0, 'x').rows, Block(place, 1, 'x').rows
    per_row = 6 * CHUNKS
    z_gather, z_sum, g_gather, y_gather, y_sum = (place.slots(per_row) for _ in range(5))
    n0, e = (Spreads(place, rows0, n0e, z_gather) for _ in range(2))
    o, d0 = (Rows(place, rows0, part, held, z_sum) for _ in range(2))
    g = Spreads(place, rows1, ga, g_gather)
    n = Spreads(place, rows1, n1, y_gather)
    d1 = Rows(place, rows1, part, held, y_sum)
    shards = (wg, wi, wo)
    w0_slots, w0_local = place.slots(24), place.local_slots(6)
    w0 = Weights(place, Block(place, 0, HEAVY['w0']), shards, dab, (w0g, w0i, w0o), w0_slots, w0_local)
    v0 = Weights(place, Block(place, 0, HEAVY['v0']), shards, held_0, (w0g, w0i, w0o), w0_slots, w0_local)
    w1 = Weights(place, Block(place, 1, HEAVY['w1']), shards, held_1, (w1g, w1i, w1o), place.slots(24), place.local_slots(6))
    bufs, outs = (mine, held1, held2, sum2), (gg, gi, go)

    def grads(b, m, part, kit, heavy):
        return Grads(place, Block(place, b, heavy), m, part, bufs, kit, outs[m], place.slots(17), place.local_slots(1))
    out1, gate1, inn1 = grads(1, 2, d_a, 0, HEAVY['out1']), grads(1, 0, d_b, 1, HEAVY['gate1']), grads(1, 1, d_a, 2, HEAVY['inn1'])
    out0, gate0, inn0 = grads(0, 2, d_b, 3, HEAVY['out0']), grads(0, 0, d_a, 0, HEAVY['gate0']), grads(0, 1, d_b, 1, HEAVY['inn0'])
    x_copy = place.local(x_in.at[c], xs, place.local_slots(1))
    g_copy = place.local(g_in.at[c], ga.at[:, y], place.local_slots(1))
    save = place.local_slots(8)
    n_save, n_load = place.local(n0e, n_out, save + 6), place.local(n_out, n1, save + 6)
    u_load = place.local(u_out, u_s, save + 7)

    def saves(k):
        slot = k % 2
        at = save + 3 * slot
        return place.local(a_s.at[slot], a_out.at[k], at), place.local(b_s.at[slot], b_out.at[k], at + 1), place.local(u_s.at[k], u_out.at[k], at + 2)

    def loads(k):
        slot = k % 2
        at = save + 3 * slot
        return place.local(a_out.at[k], a_s.at[slot], at), place.local(b_out.at[k], b_s.at[slot], at + 1)

    def start(copies):
        for copy in copies:
            copy.start()

    def wait(copies):
        for copy in copies:
            copy.wait()

    def forward(k):
        if k >= 2:
            wait(saves(k - 2))
        pre_acts(n0e, k, w0g, w0i, a_s, b_s, k % 2)
        hidden(a_s, b_s, k % 2, u_s, k)
        start(saves(k))
        project(u_s, k, w0o, part)

    def close_o(k):
        o(k).finish()

        def step(h, rows):
            total = o.total(k, h, rows).astype(BF16).astype(F32)
            out = (xs[k, h, rows].astype(F32) + total).astype(BF16)
            hs[k, h, rows] = out
            n1[k, y, h, rows] = rms(out.astype(F32))
        by_rows(step)
        n(k).start()

    def middle(k):
        n(k).finish()
        pre_acts(n1, k, w1g, w1i, a_s, b_s, k % 2)
        hidden(a_s, b_s, k % 2, u_s, k)
        hidden_back(ga, k, w1o, part, a_s, b_s, k % 2, dab)
        input_back(dab, k, w1g, w1i, part)

    def close_1(k):
        d1(k).finish()

        def step(h, rows):
            dn = d1.total(k, h, rows)
            n0e[k, z, h, rows] = cotangent(hs[k, h, rows].astype(F32), ga[k, y, h, rows].astype(F32), dn)
        by_rows(step)
        e(k).start()

    def back_hidden(k):
        e(k).finish()
        wait(loads(k))
        hidden_back(n0e, k, w0o, part, a_s, b_s, k % 2, dab)
        if k < 2:
            start(loads(k + 2))

    def back_input(k):
        input_back(dab, k, w0g, w0i, part)
        d0(k).start()

    def close_0(k):
        d0(k).finish()

        def step(h, rows):
            dn = d0.total(k, h, rows)
            hs[k, h, rows] = cotangent(xs[k, h, rows].astype(F32), n0e[k, z, h, rows].astype(F32), dn)
        by_rows(step)

    x_copy.start()
    g_copy.start()
    barrier = pltpu.get_barrier_semaphore()
    place.signal(barrier)
    place.wait(barrier)
    w0.send()
    w1.send()
    x_copy.wait()

    def start_n0(k):
        def norm(h, rows):
            n0e[k, z, h, rows] = rms(xs[k, h, rows].astype(F32))
        by_rows(norm)
        n0(k).start()
    loop(CHUNKS, start_n0)
    w0.step1()
    n0(0).relay()
    w0.step2()
    n0(1).relay()
    w0.step3()
    n0(2).relay()
    n0(3).relay()
    w1.step1()
    w0.step4()
    loop(CHUNKS, lambda k: n0(k).finish())
    n_save.start()
    w1.step2()
    w0.step5()
    g_copy.wait()
    loop(CHUNKS, lambda k: g(k).start())
    w1.step3()
    w0.step6()
    w0.done()

    forward(0)
    o(0).start()
    forward(1)
    g(0).relay()
    g(1).relay()
    o(0).relay()
    o(1).start()
    forward(2)
    g(2).relay()
    w1.step4()
    g(3).relay()
    close_o(0)
    o(1).relay()
    o(2).start()
    forward(3)
    n_save.wait()
    place.signal(phase.at[0])
    v0.send()
    n(0).relay()
    w1.step5()
    o(2).relay()
    o(3).start()
    loop(CHUNKS, lambda k: g(k).finish())
    wait(saves(2))
    wait(saves(3))
    w1.step6()
    close_o(1)
    w1.done()

    middle(0)
    n(1).relay()
    d1(0).start()
    o(3).relay()
    v0.step1()
    close_o(2)
    middle(1)
    n(2).relay()
    d1(0).relay()
    d1(1).start()
    v0.step2()
    close_o(3)
    middle(2)
    n(3).relay()
    d1(1).relay()
    d1(2).start()
    place.wait(phase.at[0])
    v0.step3()
    start(loads(0))
    close_1(0)
    middle(3)
    d1(2).relay()
    d1(3).start()
    start(loads(1))
    e(0).relay()
    v0.step4()
    weight_grad(u_s, ga, d_a)
    out1.swap()
    u_load.start()
    close_1(1)
    weight_grad_of(n1, dab, 0, d_b)
    gate1.swap()
    d1(3).relay()
    v0.step5()
    out1.combine()
    out1.first.start()
    e(1).relay()
    weight_grad_of(n1, dab, GROUPS, d_a)
    inn1.swap()
    n_load.start()
    close_1(2)
    gate1.combine()
    v0.step6()
    close_1(3)
    v0.done()

    e(2).relay()
    back_hidden(0)
    e(3).relay()
    inn1.combine()
    gate1.first.start()
    back_hidden(1)
    out1.first.relay()
    back_hidden(2)
    u_load.wait()
    n_load.wait()
    inn1.first.start()
    e(3).finish()
    weight_grad(u_s, n0e, d_b)
    out0.swap()
    gate1.first.relay()
    wait(loads(3))
    hidden_back(n0e, 3, w0o, part, a_s, b_s, 1, dab)
    out1.turn()
    weight_grad_of(n1, dab, 0, d_a)
    out0.combine()
    out0.first.start()
    back_input(0)
    inn1.first.relay()
    weight_grad_of(n1, dab, GROUPS, d_b)
    out1.second.relay()
    back_input(1)
    d0(0).relay()
    out0.first.relay()
    out1.last()
    gate1.turn()
    back_input(2)
    d0(1).relay()
    out1.done()
    place.signal(phase.at[1])
    back_input(3)
    gate1.second.relay()
    d0(2).relay()
    place.wait(phase.at[1])
    gate0.swap()
    inn1.turn()
    gate0.combine()
    gate0.first.start()
    gate1.last()
    out0.turn()
    gate1.done()
    place.signal(phase.at[2])
    inn1.second.relay()
    close_0(0)
    d0(3).relay()
    place.wait(phase.at[2])
    inn0.swap()
    gate0.first.relay()
    out0.second.relay()
    inn0.combine()
    inn0.first.start()
    inn1.last()
    close_0(1)
    gate0.turn()
    inn0.first.relay()
    close_0(2)
    out0.last()
    close_0(3)
    dx_slot, dx_local = place.slots(1), place.local_slots(1)
    dx_away, dx_here = place.remote(hs, dx_out.at[c], place.partner, dx_slot), place.local(hs, dx_out.at[c], dx_local)
    dx_away.start()
    dx_here.start()
    gate0.second.relay()
    inn0.turn()
    gate0.last()
    inn1.done()
    inn0.second.relay()
    inn0.last()
    dx_away.wait()
    dx_here.wait()
    out0.done()
    gate0.done()
    inn0.done()


VM = pl.BlockSpec(memory_space=pltpu.VMEM)
ANY = pl.BlockSpec(memory_space=pl.ANY)


def sds(shape, dtype):
    return jax.ShapeDtypeStruct(shape, dtype)


ALL_ROWS = (CHUNKS, 4, 2, HALF, WIDE)
OWN_ROWS = (CHUNKS, 2, HALF, WIDE)
FLAT_ROWS = (CHUNKS, ROWS, WIDE)
WEIGHT = (4, 4, 4, 16, WIDE)
STAGED = (4, 24, 16, WIDE)
OUTS = [
    sds((2,) + OWN_ROWS, BF16), sds((16, 4 * WIDE), F32), sds((16, 4 * WIDE), F32), sds((4, 16, WIDE), F32),
    sds(FLAT_ROWS, F32), sds(FLAT_ROWS, F32), sds(FLAT_ROWS, BF16), sds(ALL_ROWS, BF16),
    sds(STAGED, BF16), sds(STAGED, BF16),
]
SCRATCH = (
    [pltpu.VMEM(OWN_ROWS, BF16)] * 2
    + [pltpu.VMEM(ALL_ROWS, BF16)] * 3
    + [pltpu.VMEM(FLAT_ROWS, BF16)]
    + [pltpu.VMEM((2, ROWS, WIDE), F32)] * 2
    + [pltpu.VMEM((CHUNKS, 2 * GROUPS, STEP, WIDE), BF16)]
    + [pltpu.VMEM(ALL_ROWS, F32), pltpu.VMEM((3,) + OWN_ROWS, F32)]
    + [pltpu.VMEM(WEIGHT, BF16)] * 6
    + [pltpu.VMEM(WEIGHT, F32)] * 2
    + [
        pltpu.VMEM((4, 4, 4, 2, 16, WIDE), F32),
        pltpu.VMEM((4, 3, 2, 2, 2, 16, WIDE), F32),
        pltpu.VMEM((4, 3, 2, 16, WIDE), F32),
        pltpu.VMEM((4, 2, 16, WIDE), F32),
    ]
    + [pltpu.SemaphoreType.DMA((N_REMOTE,)), pltpu.SemaphoreType.DMA((N_REMOTE,)), pltpu.SemaphoreType.DMA((N_LOCAL,))]
    + [pltpu.SemaphoreType.REGULAR((3,))]
)


def call(*operands):
    return pl.pallas_call(
        kernel,
        out_shape=OUTS,
        in_specs=[ANY] * 2 + [VM] * 3,
        out_specs=[ANY] * len(OUTS),
        scratch_shapes=SCRATCH,
        compiler_params=pltpu.CompilerParams(collective_id=1, has_side_effects=True, vmem_limit_bytes=67043328),
        name='kernel_all',
    )(*operands)


def solution(mesh):
    act_spec = P(None, 'data', None, None)
    weight_spec = P('stage', None, 'data', None)

    def per_device(x, g, w_gate, w_in, w_out):
        shards = (w_gate.reshape(16, 4 * WIDE), w_in.reshape(16, 4 * WIDE), w_out.reshape(4, 16, WIDE))
        dx, d_gate, d_in, d_out, *_ = call(x.reshape((2,) + OWN_ROWS), g.reshape((2,) + OWN_ROWS), *shards)
        return dx.reshape(x.shape), d_gate.reshape(w_gate.shape), d_in.reshape(w_in.shape), d_out.reshape(w_out.shape)

    return jax.shard_map(per_device, mesh=mesh, in_specs=(act_spec, act_spec, weight_spec, weight_spec, weight_spec), out_specs=(act_spec, weight_spec, weight_spec, weight_spec), check_vma=False)
```

```python
import functools

import jax
import jax.numpy as jnp
from jax import lax
from jax.experimental import pallas as pl
from jax.experimental.pallas import tpu as pltpu
from jax.sharding import PartitionSpec as P

MESH = pl.DeviceIdType.MESH
BF16 = jnp.bfloat16
F32 = jnp.float32
RING = 4
CHUNKS = 4
HALF = 128 // CHUNKS
ROWS = 8 * HALF
STEP = 16
GROUPS = ROWS // STEP
COLS = 512
WIDE = 1024
N_REMOTE = 280
N_LOCAL = 40


class Place:
    def __init__(self, ssem, rsem, lsem, phase):
        d = lax.axis_index('data')
        self.c = lax.axis_index('stage')
        self.z, self.y, self.x = d // 16, (d // 4) % 4, d % 4
        self.ssem, self.rsem, self.lsem, self.phase = ssem, rsem, lsem, phase
        self.n_slots = self.n_local = 0
        self.partner = self.dev(self.z, self.y, self.x, 1 - self.c)

    @staticmethod
    def dev(z, y, x, c):
        return (z * 16 + y * 4 + x, c)

    def slots(self, n):
        self.n_slots += n
        assert self.n_slots <= N_REMOTE
        return self.n_slots - n

    def local_slots(self, n):
        self.n_local += n
        assert self.n_local <= N_LOCAL
        return self.n_local - n

    def local(self, src, dst, slot):
        return pltpu.make_async_copy(src, dst, self.lsem.at[slot])

    def remote(self, src, dst, dev, slot):
        return pltpu.make_async_remote_copy(src_ref=src, dst_ref=dst, send_sem=self.ssem.at[slot], recv_sem=self.rsem.at[slot], device_id=dev, device_id_type=MESH)

    def peers(self):
        z, y, x, c = self.z, self.y, self.x, self.c
        peers = [self.partner, self.dev(z, y, (x + 1) % 4, c), self.dev(z, y, (x + 3) % 4, c)]
        for step in range(1, 4):
            for core in (c, 1 - c):
                peers.append(self.dev((z + step) % 4, y, x, core))
                peers.append(self.dev(z, (y + step) % 4, x, core))
        return peers

    def signal(self, sem):
        for peer in self.peers():
            pl.semaphore_signal(sem, inc=1, device_id=peer, device_id_type=MESH)

    def wait(self, sem):
        pl.semaphore_wait(sem, len(self.peers()))


class Block:
    def __init__(self, place, b, heavy):
        self.b, self.c, self.x = b, place.c, place.x
        self.t, self.w = (place.z, place.y) if b == 0 else (place.y, place.z)
        self.heavy = heavy
        t, w, x, c = self.t, self.w, self.x, self.c
        self.a1, self.a2 = self.order(w, x, c)
        self.rows = (t, self.dev((t + 1) % 4, w, x, c), self.dev((t + 3) % 4, w, x, c))
        v = self.turned(c)
        k = 1 - v
        self.ring1 = (self.a1, self.dev(t, (w + v) % 4, (x + k) % 4, c), self.dev(t, (w + 3 * v) % 4, (x + 3 * k) % 4, c))
        self.ring2 = (self.a2, self.dev(t, (w + k) % 4, (x + v) % 4, c), self.dev(t, (w + 3 * k) % 4, (x + 3 * v) % 4, c))

    def dev(self, t, w, x, c):
        return Place.dev(t, w, x, c) if self.b == 0 else Place.dev(w, t, x, c)

    def turned(self, core):
        return core if self.heavy == 'split' else int(self.heavy == 'w')

    def order(self, w, x, core):
        v = self.turned(core)
        return (1 - v) * x + v * w, (1 - v) * w + v * x

    def place(self, a1, a2, core):
        v = self.turned(core)
        return (1 - v) * a2 + v * a1, (1 - v) * a1 + v * a2

    def index(self, m, w, x, q):
        return (w, x, q) if m == 2 else (q, w, x) if self.b == 0 else (w, q, x)

    def pieces(self, position):
        if self.b == 0:
            return [(pl.ds(pl.multiple_of(position * WIDE, WIDE), WIDE), pl.ds(0, WIDE))]
        return [(pl.ds(pl.multiple_of(u * WIDE + position * 256, 256), 256), pl.ds(u * 256, 256)) for u in range(4)]


def pair(core):
    return pl.ds(2 * core, 2)


class Gather:
    def __init__(self, place, ring, at, base):
        self.pl, self.at, self.base = place, at, base
        self.me, self.plus, self.minus = ring

    def copy(self, i):
        me = self.me
        before, after = (me + 3) % 4, (me + 1) % 4
        j, h, dev = (
            (me, 0, self.plus), (me, 1, self.minus), (me, 1, self.plus), (me, 0, self.minus), (before, 0, self.plus), (after, 1, self.minus),
        )[i]
        return self.pl.remote(self.at(j, h), self.at(j, h), dev, self.base + i)

    def start(self):
        for i in range(4):
            self.copy(i).start()

    def relay(self):
        for i in range(2):
            self.copy(i).wait_recv()
            self.copy(4 + i).start()

    def near(self):
        self.copy(2).wait_recv()
        self.copy(3).wait_recv()

    def far(self):
        self.copy(4).wait_recv()
        self.copy(5).wait_recv()
        for i in range(6):
            self.copy(i).wait_send()

    def finish(self):
        self.near()
        self.far()


class Reduce:
    def __init__(self, place, ring, own, held, add, base):
        self.pl, self.own, self.held, self.add, self.base = place, own, held, add, base
        self.me, self.plus, self.minus = ring

    def copy(self, i):
        me, own, held = self.me, self.own, self.held
        far, after, before = (me + 2) % 4, (me + 1) % 4, (me + 3) % 4
        if i == 0:
            src, dst = own(far, 0), held(0).at[0]
        elif i == 1:
            src, dst = own(far, 1), held(0).at[1]
        elif i == 2:
            src, dst = own(after, 1), held(1).at[1]
        elif i == 3:
            src, dst = own(before, 0), held(2).at[0]
        elif i == 4:
            src, dst = held(0).at[0], held(1).at[0]
        else:
            src, dst = held(0).at[1], held(2).at[1]
        return self.pl.remote(src, dst, self.minus if i % 2 else self.plus, self.base + i)

    def start(self):
        for i in range(4):
            self.copy(i).start()

    def relay(self):
        for i in range(2):
            self.copy(i).wait_recv()
            self.add(i, (self.me + 3) % 4 if i else (self.me + 1) % 4)
            self.copy(4 + i).start()

    def finish(self):
        for i in range(2, 6):
            self.copy(i).wait_recv()
        for i in range(6):
            self.copy(i).wait_send()


def loop(n, body, start=0):
    def one(i, carry):
        body(i)
        return carry
    lax.fori_loop(start, n, one, 0)


def by_rows(body):
    def one(i):
        body(i // (HALF // STEP), pl.ds(pl.multiple_of(i % (HALF // STEP) * STEP, STEP), STEP))
    loop(2 * HALF // STEP, one)


def inverse_rms(rows):
    return lax.rsqrt(jnp.mean(rows * rows, axis=-1, keepdims=True) + 1e-6)


def rms(rows):
    return (rows * inverse_rms(rows)).astype(BF16)


def cotangent(h, e, dn):
    r = inverse_rms(h)
    back = r * dn - h * (r * r * r * jnp.mean(h * dn, axis=-1, keepdims=True))
    return (e + back).astype(BF16)


class Rows:
    def __init__(self, place, ring, part, held, base):
        self.pl, self.ring, self.part, self.held, self.base = place, ring, part, held, base

    def __call__(self, k):
        part, held = self.part, self.held

        def add(h, j):
            def one(i):
                rows = pl.ds(pl.multiple_of(i * STEP, STEP), STEP)
                held[0, k, h, rows] = held[0, k, h, rows] + part[k, j, h, rows]
            loop(HALF // STEP, one)
        return Reduce(self.pl, self.ring, lambda j, h: part.at[k, j, h], lambda b: held.at[b, k], add, self.base + 6 * k)

    def total(self, k, h, rows):
        return self.part[k, self.ring[0], h, rows] + self.held[1, k, h, rows] + self.held[2, k, h, rows]


class Spreads:
    def __init__(self, place, ring, ref, base):
        self.pl, self.ring, self.ref, self.base = place, ring, ref, base

    def __call__(self, k):
        return Gather(self.pl, self.ring, lambda j, h: self.ref.at[k, j, h], self.base + 6 * k)


class Weights:
    def __init__(self, place, block, shards, held, outs, base, local):
        self.pl, self.bk, self.s, self.shards, self.held, self.outs = place, block, block.b, shards, held, outs
        self.slots, self.out_slot, self.swap_slots = base, base + 8, base + 9
        self.local, self.copy_local = local, local + 3
        self.first = Gather(place, block.ring2, lambda j, h: held.at[block.a1, pl.ds((2 * j + h) * 3, 3)], base + 12)
        self.second = Gather(place, block.ring1, lambda j, h: held.at[j, 12 * h:12 * h + 12], base + 18)

    def piece(self, a1, a2, q, m):
        return self.held.at[a1, (2 * a2 + q) * 3 + m]

    def parts(self, dz):
        bk = self.bk
        target = (bk.t + dz) % 4
        core = bk.t // 2
        a1, a2 = bk.order(bk.w, bk.x, core)
        for m in range(2):
            whole = self.piece(a1, a2, bk.t % 2, m)
            copies = [(self.shards[m].at[:, src], whole.at[:, dst]) for src, dst in bk.pieces(target)]
            yield m, copies, whole, bk.dev(target, bk.w, bk.x, core)

    def out_part(self, core):
        a1, a2 = self.bk.order(self.bk.w, self.bk.x, core)
        copies = [(self.shards[2].at[2 * core + q], self.piece(a1, a2, q, 2)) for q in range(2)]
        return copies, self.held.at[a1, pl.ds(0, 2)]

    def source(self, wait):
        place, s = self.pl, self.s
        mine = self.bk.t // 2 == s

        def away(copies, whole, dev, slot):
            if wait:
                place.remote(whole, whole, dev, slot).wait_send()
                return
            for src, dst in copies:
                place.remote(src, dst, dev, slot).start()

        def here(copies, whole, slot):
            if wait:
                place.local(whole, whole, slot).wait()
                return
            for src, dst in copies:
                place.local(src, dst, slot).start()

        @pl.when(place.c == s)
        def _():
            for dz in range(1, 4):
                for m, copies, whole, dev in self.parts(dz):
                    away(copies, whole, dev, self.slots + 2 * dz + m)

            @pl.when(mine)
            def _():
                for m, copies, whole, _ in self.parts(0):
                    here(copies, whole, self.local + m)

            @pl.when(jnp.logical_not(mine))
            def _():
                for m, copies, whole, _ in self.parts(0):
                    away(copies, whole, place.partner, self.slots + m)
            here(*self.out_part(s), self.local + 2)
            away(*self.out_part(1 - s), place.partner, self.out_slot)

    def send(self):
        self.source(False)

    def arrive(self):
        place, bk, s = self.pl, self.bk, self.s
        for dz in range(4):
            source = (bk.t + 4 - dz) % 4
            here = source // 2 == place.c
            if dz == 0:
                here = jnp.logical_and(here, place.c != s)

            @pl.when(here)
            def _(dz=dz, source=source):
                for m in range(2):
                    dst = self.piece(bk.a1, bk.a2, source % 2, m)
                    place.remote(dst, dst, place.partner, self.slots + 2 * dz + m).wait_recv()

        self.source(True)

        @pl.when(place.c != s)
        def _():
            _, whole = self.out_part(1 - s)
            place.remote(whole, whole, place.partner, self.out_slot).wait_recv()

    def spread(self, a1):
        place, bk = self.pl, self.bk

        def one(a2):
            w, x = bk.place(a1, a2, place.c)
            for m in range(3):
                for q in range(2):
                    src = self.piece(a1, a2, q, m)
                    dst = self.outs[m].at[bk.index(m, w, x, 2 * place.c + q)]
                    place.remote(src, dst, place.partner, self.swap_slots + m).start()
                    place.local(src, dst, self.copy_local + m).start()
        loop(4, one)

    def done(self):
        place, bk = self.pl, self.bk
        every = slice(None)
        for m in range(3):
            mine, other = (self.outs[m].at[bk.index(m, every, every, pair(core))] for core in (place.c, 1 - place.c))
            place.remote(mine, other, place.partner, self.swap_slots + m).wait_recv()
            place.remote(mine, other, place.partner, self.swap_slots + m).wait_send()
            place.local(mine, mine, self.copy_local + m).wait()

    def step1(self):
        self.arrive()
        self.first.start()

    def step2(self):
        self.first.relay()

    def step3(self):
        self.first.finish()
        self.second.start()
        self.spread(self.bk.a1)

    def step4(self):
        self.second.relay()

    def step5(self):
        self.second.near()
        self.spread((self.bk.a1 + 3) % 4)
        self.spread((self.bk.a1 + 1) % 4)

    def step6(self):
        self.second.far()
        self.spread((self.bk.a1 + 2) % 4)


class Grads:
    def __init__(self, place, block, m, part, kit, out, base, local):
        self.pl, self.bk, self.s, self.m, self.part, self.out = place, block, block.b, m, part, out
        mine, held1, held2, sum2 = kit
        self.mine, self.held1, self.held2, self.sum2 = mine, held1, held2, sum2
        self.local = local
        self.swap_slot, self.hand_slots = base, base + 1

        def add1(h, j):
            def one(i):
                k, q = i // 2, i % 2
                held1[0, h, k, q] = held1[0, h, k, q] + mine[j, 2 * h + k, q]
            loop(4, one)
        self.first = Reduce(place, block.ring1, lambda j, h: mine.at[j, 2 * h:2 * h + 2], lambda b: held1.at[b], add1, base + 5)

        def add2(h, j):
            held2[0, h] = held2[0, h] + mine[block.a1, j, h]
        self.second = Reduce(place, block.ring2, lambda j, h: mine.at[block.a1, j, h], lambda b: held2.at[b], add2, base + 11)

    def swap(self):
        place, bk = self.pl, self.bk

        def one(p):
            w, x, other = p // 4, p % 4, 1 - place.c
            a1, a2 = bk.order(w, x, other)
            src = self.part.at[bk.index(self.m, w, x, pair(other))]
            place.remote(src, self.mine.at[a1, a2], place.partner, self.swap_slot).start()
        loop(16, one)

    def combine(self):
        place, bk, mine = self.pl, self.bk, self.mine
        whole = place.remote(mine, mine, place.partner, self.swap_slot)
        whole.wait_recv()

        def one(p):
            w, x = p // 4, p % 4
            a1, a2 = bk.order(w, x, place.c)
            for q in range(2):
                mine[a1, a2, q] = mine[a1, a2, q] + self.part[bk.index(self.m, w, x, 2 * place.c + q)]
        loop(16, one)
        whole.wait_send()

    def turn(self):
        bk, mine, held1 = self.bk, self.mine, self.held1
        self.first.finish()

        def one(i):
            h, k, q = i // 4, i // 2 % 2, i % 2
            mine[bk.a1, i // 2, q] = mine[bk.a1, i // 2, q] + held1[1, h, k, q] + held1[2, h, k, q]
        loop(8, one)
        self.second.start()

    def last(self):
        self.second.finish()
        for h in range(2):
            self.sum2[h] = self.mine[self.bk.a1, self.bk.a2, h] + self.held2[1, h] + self.held2[2, h]
        self.hand(False)

    def hand(self, wait):
        place, bk, s = self.pl, self.bk, self.s
        to_self = place.c == s

        def stay(copies, whole):
            if wait:
                place.local(whole, whole, self.local).wait()
                return
            for src, dst in copies:
                place.local(src, dst, self.local).start()

        def go(copies, whole, dev, slot):
            if wait:
                place.remote(whole, whole, dev, slot).wait_send()
                return
            for src, dst in copies:
                place.remote(src, dst, dev, slot).start()

        if self.m == 2:
            copies = [(self.sum2, self.out.at[pair(place.c)])]
            pl.when(to_self)(lambda: stay(copies, self.sum2))
            pl.when(jnp.logical_not(to_self))(lambda: go(copies, self.sum2, place.partner, self.hand_slots))
            return
        for dz in range(4):
            target = (bk.t + dz) % 4
            whole = self.sum2.at[target % 2]
            copies = [(self.sum2.at[target % 2, :, own], self.out.at[:, shard]) for shard, own in bk.pieces(bk.t)]
            here = target // 2 == place.c
            send = functools.partial(go, copies, whole, bk.dev(target, bk.w, bk.x, s), self.hand_slots + dz)
            if dz:
                pl.when(here)(send)
            else:
                pl.when(jnp.logical_and(here, to_self))(functools.partial(stay, copies, whole))
                pl.when(jnp.logical_and(here, jnp.logical_not(to_self)))(send)

    def done(self):
        place, bk, s = self.pl, self.bk, self.s

        def land(like, slot):
            place.remote(like, like, place.partner, slot).wait_recv()

        @pl.when(place.c == s)
        def _():
            if self.m == 2:
                land(self.sum2, self.hand_slots)
                return
            for dz in range(1, 4):
                land(self.sum2.at[0], self.hand_slots + dz)
            pl.when(bk.t // 2 != s)(lambda: land(self.sum2.at[0], self.hand_slots))
        self.hand(True)


def mm(a, b):
    return jnp.dot(a, b, preferred_element_type=F32)


def mm_nt(a, b):
    return lax.dot_general(a, b, (((1,), (1,)), ((), ())), preferred_element_type=F32)


def mm_tn(a, b):
    return lax.dot_general(a, b, (((0,), (0,)), ((), ())), preferred_element_type=F32)


def chunk(ref, k):
    return ref[k].reshape(ROWS, WIDE)


def square(ref):
    return ref[...].reshape(WIDE, WIDE)


def pre_acts(n_ref, k, gate, inn, a_ref, b_ref, slot):
    a_ref[slot] = mm(chunk(n_ref, k), square(gate))
    b_ref[slot] = mm(chunk(n_ref, k), square(inn))


def hidden(a_ref, b_ref, slot, u_ref, k):
    def one(i):
        rows = pl.ds(pl.multiple_of(i * STEP, STEP), STEP)
        a = a_ref[slot, rows]
        u_ref[k, rows] = (a * jax.nn.sigmoid(a) * b_ref[slot, rows]).astype(BF16)
    loop(ROWS // STEP, one)


def project(u_ref, k, out, part):
    part[k] = mm(u_ref[k], square(out)).reshape(4, 2, HALF, WIDE)


def hidden_back(e_ref, k, out, t_ref, a_ref, b_ref, slot, dab):
    t_ref[k] = mm_nt(chunk(e_ref, k), square(out)).reshape(4, 2, HALF, WIDE)
    per_half = HALF // STEP

    def one(i):
        rows = pl.ds(pl.multiple_of(i * STEP, STEP), STEP)
        j = i // (2 * per_half)
        h = i // per_half % 2
        t = t_ref[k, j, h, pl.ds(pl.multiple_of(i % per_half * STEP, STEP), STEP)]
        a, b = a_ref[slot, rows], b_ref[slot, rows]
        s = jax.nn.sigmoid(a)
        dab[k, i] = (t * b * s * (1.0 + a * (1.0 - s))).astype(BF16)
        dab[k, GROUPS + i] = (t * a * s).astype(BF16)
    loop(ROWS // STEP, one)


def input_back(dab, k, gate, inn, part):
    def one(i):
        da, db = dab[k, :GROUPS].reshape(ROWS, WIDE), dab[k, GROUPS:].reshape(ROWS, WIDE)
        cols = pl.ds(pl.multiple_of(i * COLS, COLS), COLS)
        dn = mm_nt(da, gate[pl.ds(2 * i, 2)].reshape(COLS, WIDE)) + mm_nt(db, inn[pl.ds(2 * i, 2)].reshape(COLS, WIDE))
        part[k, :, :, :, cols] = dn.reshape(4, 2, HALF, COLS)
    loop(WIDE // COLS, one)


def weight_grad(lhs, rhs, out):
    def one(i):
        cols = pl.ds(pl.multiple_of(i * 256, 256), 256)
        left = lhs[..., cols].reshape(CHUNKS * ROWS, 256)
        out[i] = mm_tn(left, rhs[...].reshape(CHUNKS * ROWS, WIDE)).reshape(4, 4, 16, WIDE)
    loop(4, one)


def weight_grad_of(n_ref, dab, first, out):
    def one(i):
        cols = pl.ds(pl.multiple_of(i * 256, 256), 256)
        right = dab[:, first:first + GROUPS].reshape(CHUNKS * ROWS, WIDE)
        out[i] = mm_tn(n_ref[..., cols].reshape(CHUNKS * ROWS, 256), right).reshape(4, 4, 16, WIDE)
    loop(4, one)


HEAVY = {'w0': 'split', 'w1': 'x', 'v0': 'x', 'out1': 'x', 'gate1': 'split', 'in1': 'split', 'out0': 'split', 'gate0': 'split', 'in0': 'split'}


def kernel(x_in, g_in, wg, wi, wo, dx_out, gg, gi, go, a_out, b_out, u_out, n_out, held_1, held_0,
           xs, hs, n0e, n1, ga, u_s, a_s, b_s, dab, part, held, w0g, w0i, w0o, w1g, w1i, w1o,
           d_a, d_b, mine, held1, held2, sum2, ssem, rsem, lsem, phase):
    place = Place(ssem, rsem, lsem, phase)
    z, y, c = place.z, place.y, place.c
    rows0, rows1 = Block(place, 0, 'x').rows, Block(place, 1, 'x').rows
    per_row = 6 * CHUNKS
    z_gather, z_sum, g_gather, y_gather, y_sum = (place.slots(per_row) for _ in range(5))
    n0, e = (Spreads(place, rows0, n0e, z_gather) for _ in range(2))
    o, d0 = (Rows(place, rows0, part, held, z_sum) for _ in range(2))
    g = Spreads(place, rows1, ga, g_gather)
    n = Spreads(place, rows1, n1, y_gather)
    d1 = Rows(place, rows1, part, held, y_sum)
    shards = (wg, wi, wo)
    w0_slots, w0_local = place.slots(24), place.local_slots(6)
    w0 = Weights(place, Block(place, 0, HEAVY['w0']), shards, dab, (w0g, w0i, w0o), w0_slots, w0_local)
    v0 = Weights(place, Block(place, 0, HEAVY['v0']), shards, held_0, (w0g, w0i, w0o), w0_slots, w0_local)
    w1 = Weights(place, Block(place, 1, HEAVY['w1']), shards, held_1, (w1g, w1i, w1o), place.slots(24), place.local_slots(6))
    outs = gg, gi, go

    def grads(b, m, part, own, ring):
        name = ('gate', 'in', 'out')[m] + str(b)
        kit = mine.at[own], held1.at[ring], held2.at[own], sum2.at[own]
        return Grads(place, Block(place, b, HEAVY[name]), m, part, kit, outs[m], place.slots(17), place.local_slots(1))
    out1, gate1, inn1 = grads(1, 2, d_a, 0, 0), grads(1, 0, d_b, 1, 1), grads(1, 1, d_a, 2, 2)
    out0, gate0, inn0 = grads(0, 2, d_b, 3, 3), grads(0, 0, d_a, 4, 0), grads(0, 1, d_b, 0, 1)
    x_copy = place.local(x_in.at[c], xs, place.local_slots(1))
    g_copy = place.local(g_in.at[c], ga.at[:, y], place.local_slots(1))
    save = place.local_slots(8)
    n_save, n_load = place.local(n0e, n_out, save + 6), place.local(n_out, n1, save + 6)
    u_load = place.local(u_out, u_s, save + 7)

    def saves(k):
        slot = k % 2
        at = save + 3 * slot
        return place.local(a_s.at[slot], a_out.at[k], at), place.local(b_s.at[slot], b_out.at[k], at + 1), place.local(u_s.at[k], u_out.at[k], at + 2)

    def loads(k):
        slot = k % 2
        at = save + 3 * slot
        return place.local(a_out.at[k], a_s.at[slot], at), place.local(b_out.at[k], b_s.at[slot], at + 1)

    def start(copies):
        for copy in copies:
            copy.start()

    def wait(copies):
        for copy in copies:
            copy.wait()

    def forward(k):
        if k >= 2:
            wait(saves(k - 2))
        pre_acts(n0e, k, w0g, w0i, a_s, b_s, k % 2)
        hidden(a_s, b_s, k % 2, u_s, k)
        start(saves(k))
        project(u_s, k, w0o, part)

    def close_o(k):
        o(k).finish()

        def step(h, rows):
            total = o.total(k, h, rows).astype(BF16).astype(F32)
            out = (xs[k, h, rows].astype(F32) + total).astype(BF16)
            hs[k, h, rows] = out
            n1[k, y, h, rows] = rms(out.astype(F32))
        by_rows(step)
        n(k).start()

    def middle(k):
        n(k).finish()
        pre_acts(n1, k, w1g, w1i, a_s, b_s, k % 2)
        hidden(a_s, b_s, k % 2, u_s, k)
        hidden_back(ga, k, w1o, part, a_s, b_s, k % 2, dab)
        input_back(dab, k, w1g, w1i, part)

    def close_1(k):
        d1(k).finish()

        def step(h, rows):
            dn = d1.total(k, h, rows)
            n0e[k, z, h, rows] = cotangent(hs[k, h, rows].astype(F32), ga[k, y, h, rows].astype(F32), dn)
        by_rows(step)
        e(k).start()

    def back_hidden(k):
        e(k).finish()
        wait(loads(k))
        hidden_back(n0e, k, w0o, part, a_s, b_s, k % 2, dab)
        if k < 2:
            start(loads(k + 2))

    def back_input(k):
        input_back(dab, k, w0g, w0i, part)
        d0(k).start()

    def close_0(k):
        d0(k).finish()

        def step(h, rows):
            dn = d0.total(k, h, rows)
            hs[k, h, rows] = cotangent(xs[k, h, rows].astype(F32), n0e[k, z, h, rows].astype(F32), dn)
        by_rows(step)

    x_copy.start()
    g_copy.start()
    barrier = pltpu.get_barrier_semaphore()
    place.signal(barrier)
    place.wait(barrier)
    w0.send()
    w1.send()
    x_copy.wait()

    def start_n0(k):
        def norm(h, rows):
            n0e[k, z, h, rows] = rms(xs[k, h, rows].astype(F32))
        by_rows(norm)
        n0(k).start()
    loop(CHUNKS, start_n0)
    w0.step1()
    n0(0).relay()
    w0.step2()
    n0(1).relay()
    w0.step3()
    n0(2).relay()
    n0(3).relay()
    w1.step1()
    w0.step4()
    loop(CHUNKS, lambda k: n0(k).finish())
    n_save.start()
    w1.step2()
    w0.step5()
    g_copy.wait()
    loop(CHUNKS, lambda k: g(k).start())
    w1.step3()
    w0.step6()
    w0.done()

    forward(0)
    o(0).start()
    forward(1)
    g(0).relay()
    g(1).relay()
    o(0).relay()
    o(1).start()
    forward(2)
    g(2).relay()
    w1.step4()
    g(3).relay()
    close_o(0)
    o(1).relay()
    o(2).start()
    forward(3)
    n_save.wait()
    place.signal(phase.at[0])
    v0.send()
    n(0).relay()
    w1.step5()
    o(2).relay()
    o(3).start()
    loop(CHUNKS, lambda k: g(k).finish())
    wait(saves(2))
    wait(saves(3))
    w1.step6()
    close_o(1)
    w1.done()

    middle(0)
    n(1).relay()
    d1(0).start()
    o(3).relay()
    v0.step1()
    close_o(2)
    middle(1)
    n(2).relay()
    d1(0).relay()
    d1(1).start()
    v0.step2()
    close_o(3)
    middle(2)
    n(3).relay()
    d1(1).relay()
    d1(2).start()
    place.wait(phase.at[0])
    v0.step3()
    start(loads(0))
    close_1(0)
    middle(3)
    d1(2).relay()
    d1(3).start()
    start(loads(1))
    e(0).relay()
    v0.step4()
    weight_grad(u_s, ga, d_a)
    out1.swap()
    u_load.start()
    close_1(1)
    weight_grad_of(n1, dab, 0, d_b)
    gate1.swap()
    d1(3).relay()
    v0.step5()
    out1.combine()
    out1.first.start()
    e(1).relay()
    weight_grad_of(n1, dab, GROUPS, d_a)
    inn1.swap()
    n_load.start()
    close_1(2)
    gate1.combine()
    v0.step6()
    close_1(3)
    v0.done()

    e(2).relay()
    back_hidden(0)
    e(3).relay()
    inn1.combine()
    gate1.first.start()
    back_hidden(1)
    out1.first.relay()
    back_hidden(2)
    u_load.wait()
    n_load.wait()
    inn1.first.start()
    e(3).finish()
    weight_grad(u_s, n0e, d_b)
    out0.swap()
    gate1.first.relay()
    wait(loads(3))
    hidden_back(n0e, 3, w0o, part, a_s, b_s, 1, dab)
    out1.turn()
    place.signal(phase.at[1])
    weight_grad_of(n1, dab, 0, d_a)
    out0.combine()
    out0.first.start()
    place.wait(phase.at[1])
    gate0.swap()
    back_input(0)
    inn1.first.relay()
    weight_grad_of(n1, dab, GROUPS, d_b)
    gate0.combine()
    gate0.first.start()
    out1.second.relay()
    back_input(1)
    d0(0).relay()
    gate1.turn()
    out1.last()
    out1.done()
    place.signal(phase.at[2])
    out0.first.relay()
    back_input(2)
    place.wait(phase.at[2])
    inn0.swap()
    d0(1).relay()
    gate1.second.relay()
    inn0.combine()
    inn0.first.start()
    back_input(3)
    inn1.turn()
    d0(2).relay()
    gate0.first.relay()
    out0.turn()
    gate1.last()
    inn1.second.relay()
    close_0(0)
    d0(3).relay()
    inn0.first.relay()
    out0.second.relay()
    gate0.turn()
    inn1.last()
    close_0(1)
    close_0(2)
    gate0.second.relay()
    out0.last()
    close_0(3)
    dx_slot, dx_local = place.slots(1), place.local_slots(1)
    dx_away, dx_here = place.remote(hs, dx_out.at[c], place.partner, dx_slot), place.local(hs, dx_out.at[c], dx_local)
    dx_away.start()
    dx_here.start()
    inn0.turn()
    gate0.last()
    gate1.done()
    inn1.done()
    inn0.second.relay()
    inn0.last()
    dx_away.wait()
    dx_here.wait()
    out0.done()
    gate0.done()
    inn0.done()


VM = pl.BlockSpec(memory_space=pltpu.VMEM)
ANY = pl.BlockSpec(memory_space=pl.ANY)


def sds(shape, dtype):
    return jax.ShapeDtypeStruct(shape, dtype)


ALL_ROWS = (CHUNKS, 4, 2, HALF, WIDE)
OWN_ROWS = (CHUNKS, 2, HALF, WIDE)
FLAT_ROWS = (CHUNKS, ROWS, WIDE)
WEIGHT = (4, 4, 4, 16, WIDE)
STAGED = (4, 24, 16, WIDE)
OUTS = [
    sds((2,) + OWN_ROWS, BF16), sds((16, 4 * WIDE), F32), sds((16, 4 * WIDE), F32), sds((4, 16, WIDE), F32),
    sds(FLAT_ROWS, F32), sds(FLAT_ROWS, F32), sds(FLAT_ROWS, BF16), sds(ALL_ROWS, BF16),
    sds(STAGED, BF16), sds(STAGED, BF16),
]
SCRATCH = (
    [pltpu.VMEM(OWN_ROWS, BF16)] * 2
    + [pltpu.VMEM(ALL_ROWS, BF16)] * 3
    + [pltpu.VMEM(FLAT_ROWS, BF16)]
    + [pltpu.VMEM((2, ROWS, WIDE), F32)] * 2
    + [pltpu.VMEM((CHUNKS, 2 * GROUPS, STEP, WIDE), BF16)]
    + [pltpu.VMEM(ALL_ROWS, F32), pltpu.VMEM((3,) + OWN_ROWS, F32)]
    + [pltpu.VMEM(WEIGHT, BF16)] * 6
    + [pltpu.VMEM(WEIGHT, F32)] * 2
    + [
        pltpu.VMEM((5, 4, 4, 2, 16, WIDE), F32),
        pltpu.VMEM((4, 3, 2, 2, 2, 16, WIDE), F32),
        pltpu.VMEM((5, 3, 2, 16, WIDE), F32),
        pltpu.VMEM((5, 2, 16, WIDE), F32),
    ]
    + [pltpu.SemaphoreType.DMA((N_REMOTE,)), pltpu.SemaphoreType.DMA((N_REMOTE,)), pltpu.SemaphoreType.DMA((N_LOCAL,))]
    + [pltpu.SemaphoreType.REGULAR((3,))]
)


def call(*operands):
    return pl.pallas_call(
        kernel,
        out_shape=OUTS,
        in_specs=[ANY] * 2 + [VM] * 3,
        out_specs=[ANY] * len(OUTS),
        scratch_shapes=SCRATCH,
        compiler_params=pltpu.CompilerParams(collective_id=1, has_side_effects=True, vmem_limit_bytes=67043328),
        name='kernel_all',
    )(*operands)


def solution(mesh):
    act_spec = P(None, 'data', None, None)
    weight_spec = P('stage', None, 'data', None)

    def per_device(x, g, w_gate, w_in, w_out):
        shards = (w_gate.reshape(16, 4 * WIDE), w_in.reshape(16, 4 * WIDE), w_out.reshape(4, 16, WIDE))
        dx, d_gate, d_in, d_out, *_ = call(x.reshape((2,) + OWN_ROWS), g.reshape((2,) + OWN_ROWS), *shards)
        return dx.reshape(x.shape), d_gate.reshape(w_gate.shape), d_in.reshape(w_in.shape), d_out.reshape(w_out.shape)

    return jax.shard_map(per_device, mesh=mesh, in_specs=(act_spec, act_spec, weight_spec, weight_spec, weight_spec), out_specs=(act_spec, weight_spec, weight_spec, weight_spec), check_vma=False)
```

```python
import functools

import jax
import jax.numpy as jnp
from jax import lax
from jax.experimental import pallas as pl
from jax.experimental.pallas import tpu as pltpu
from jax.sharding import PartitionSpec as P

MESH = pl.DeviceIdType.MESH
BF16 = jnp.bfloat16
F32 = jnp.float32
RING = 4
CHUNKS = 4
HALF = 128 // CHUNKS
ROWS = 8 * HALF
STEP = 16
GROUPS = ROWS // STEP
COLS = 512
WIDE = 1024
N_REMOTE = 280
N_LOCAL = 40


class Place:
    def __init__(self, ssem, rsem, lsem, phase):
        d = lax.axis_index('data')
        self.c = lax.axis_index('stage')
        self.z, self.y, self.x = d // 16, (d // 4) % 4, d % 4
        self.ssem, self.rsem, self.lsem, self.phase = ssem, rsem, lsem, phase
        self.n_slots = self.n_local = 0
        self.partner = self.dev(self.z, self.y, self.x, 1 - self.c)

    @staticmethod
    def dev(z, y, x, c):
        return (z * 16 + y * 4 + x, c)

    def slots(self, n):
        self.n_slots += n
        assert self.n_slots <= N_REMOTE
        return self.n_slots - n

    def local_slots(self, n):
        self.n_local += n
        assert self.n_local <= N_LOCAL
        return self.n_local - n

    def local(self, src, dst, slot):
        return pltpu.make_async_copy(src, dst, self.lsem.at[slot])

    def remote(self, src, dst, dev, slot):
        return pltpu.make_async_remote_copy(src_ref=src, dst_ref=dst, send_sem=self.ssem.at[slot], recv_sem=self.rsem.at[slot], device_id=dev, device_id_type=MESH)

    def peers(self):
        z, y, x, c = self.z, self.y, self.x, self.c
        peers = [self.partner, self.dev(z, y, (x + 1) % 4, c), self.dev(z, y, (x + 3) % 4, c)]
        for step in range(1, 4):
            for core in (c, 1 - c):
                peers.append(self.dev((z + step) % 4, y, x, core))
                peers.append(self.dev(z, (y + step) % 4, x, core))
        return peers

    def signal(self, sem):
        for peer in self.peers():
            pl.semaphore_signal(sem, inc=1, device_id=peer, device_id_type=MESH)

    def wait(self, sem):
        pl.semaphore_wait(sem, len(self.peers()))


class Block:
    def __init__(self, place, b, heavy):
        self.b, self.c, self.x = b, place.c, place.x
        self.t, self.w = (place.z, place.y) if b == 0 else (place.y, place.z)
        self.heavy = heavy
        t, w, x, c = self.t, self.w, self.x, self.c
        self.a1, self.a2 = self.order(w, x, c)
        self.rows = (t, self.dev((t + 1) % 4, w, x, c), self.dev((t + 3) % 4, w, x, c))
        v = self.turned(c)
        k = 1 - v
        self.ring1 = (self.a1, self.dev(t, (w + v) % 4, (x + k) % 4, c), self.dev(t, (w + 3 * v) % 4, (x + 3 * k) % 4, c))
        self.ring2 = (self.a2, self.dev(t, (w + k) % 4, (x + v) % 4, c), self.dev(t, (w + 3 * k) % 4, (x + 3 * v) % 4, c))

    def dev(self, t, w, x, c):
        return Place.dev(t, w, x, c) if self.b == 0 else Place.dev(w, t, x, c)

    def turned(self, core):
        return core if self.heavy == 'split' else int(self.heavy == 'w')

    def order(self, w, x, core):
        v = self.turned(core)
        return (1 - v) * x + v * w, (1 - v) * w + v * x

    def place(self, a1, a2, core):
        v = self.turned(core)
        return (1 - v) * a2 + v * a1, (1 - v) * a1 + v * a2

    def index(self, m, w, x, q):
        return (w, x, q) if m == 2 else (q, w, x) if self.b == 0 else (w, q, x)

    def pieces(self, position):
        if self.b == 0:
            return [(pl.ds(pl.multiple_of(position * WIDE, WIDE), WIDE), pl.ds(0, WIDE))]
        return [(pl.ds(pl.multiple_of(u * WIDE + position * 256, 256), 256), pl.ds(u * 256, 256)) for u in range(4)]


def pair(core):
    return pl.ds(2 * core, 2)


class Gather:
    def __init__(self, place, ring, at, base):
        self.pl, self.at, self.base = place, at, base
        self.me, self.plus, self.minus = ring

    def copy(self, i):
        me = self.me
        before, after = (me + 3) % 4, (me + 1) % 4
        j, h, dev = (
            (me, 0, self.plus), (me, 1, self.minus), (me, 1, self.plus), (me, 0, self.minus), (before, 0, self.plus), (after, 1, self.minus),
        )[i]
        return self.pl.remote(self.at(j, h), self.at(j, h), dev, self.base + i)

    def start(self):
        for i in range(4):
            self.copy(i).start()

    def relay(self):
        for i in range(2):
            self.copy(i).wait_recv()
            self.copy(4 + i).start()

    def near(self):
        self.copy(2).wait_recv()
        self.copy(3).wait_recv()

    def far(self):
        self.copy(4).wait_recv()
        self.copy(5).wait_recv()
        for i in range(6):
            self.copy(i).wait_send()

    def finish(self):
        self.near()
        self.far()


class Reduce:
    def __init__(self, place, ring, own, held, add, base):
        self.pl, self.own, self.held, self.add, self.base = place, own, held, add, base
        self.me, self.plus, self.minus = ring

    def copy(self, i):
        me, own, held = self.me, self.own, self.held
        far, after, before = (me + 2) % 4, (me + 1) % 4, (me + 3) % 4
        if i == 0:
            src, dst = own(far, 0), held(0).at[0]
        elif i == 1:
            src, dst = own(far, 1), held(0).at[1]
        elif i == 2:
            src, dst = own(after, 1), held(1).at[1]
        elif i == 3:
            src, dst = own(before, 0), held(2).at[0]
        elif i == 4:
            src, dst = held(0).at[0], held(1).at[0]
        else:
            src, dst = held(0).at[1], held(2).at[1]
        return self.pl.remote(src, dst, self.minus if i % 2 else self.plus, self.base + i)

    def start(self):
        for i in range(4):
            self.copy(i).start()

    def relay(self):
        for i in range(2):
            self.copy(i).wait_recv()
            self.add(i, (self.me + 3) % 4 if i else (self.me + 1) % 4)
            self.copy(4 + i).start()

    def finish(self):
        for i in range(2, 6):
            self.copy(i).wait_recv()
        for i in range(6):
            self.copy(i).wait_send()


def loop(n, body, start=0):
    def one(i, carry):
        body(i)
        return carry
    lax.fori_loop(start, n, one, 0)


def by_rows(body):
    def one(i):
        body(i // (HALF // STEP), pl.ds(pl.multiple_of(i % (HALF // STEP) * STEP, STEP), STEP))
    loop(2 * HALF // STEP, one)


def inverse_rms(rows):
    return lax.rsqrt(jnp.mean(rows * rows, axis=-1, keepdims=True) + 1e-6)


def rms(rows):
    return (rows * inverse_rms(rows)).astype(BF16)


def cotangent(h, e, dn):
    r = inverse_rms(h)
    back = r * dn - h * (r * r * r * jnp.mean(h * dn, axis=-1, keepdims=True))
    return (e + back).astype(BF16)


class Rows:
    def __init__(self, place, ring, part, held, base):
        self.pl, self.ring, self.part, self.held, self.base = place, ring, part, held, base

    def __call__(self, k):
        part, held = self.part, self.held

        def add(h, j):
            def one(i):
                rows = pl.ds(pl.multiple_of(i * STEP, STEP), STEP)
                held[0, k, h, rows] = held[0, k, h, rows] + part[k, j, h, rows]
            loop(HALF // STEP, one)
        return Reduce(self.pl, self.ring, lambda j, h: part.at[k, j, h], lambda b: held.at[b, k], add, self.base + 6 * k)

    def total(self, k, h, rows):
        return self.part[k, self.ring[0], h, rows] + self.held[1, k, h, rows] + self.held[2, k, h, rows]


class Spreads:
    def __init__(self, place, ring, ref, base):
        self.pl, self.ring, self.ref, self.base = place, ring, ref, base

    def __call__(self, k):
        return Gather(self.pl, self.ring, lambda j, h: self.ref.at[k, j, h], self.base + 6 * k)


class Weights:
    def __init__(self, place, block, shards, held, outs, base, local):
        self.pl, self.bk, self.s, self.shards, self.held, self.outs = place, block, block.b, shards, held, outs
        self.slots, self.out_slot, self.swap_slots = base, base + 8, base + 9
        self.local, self.copy_local = local, local + 3
        self.first = Gather(place, block.ring2, lambda j, h: held.at[block.a1, pl.ds((2 * j + h) * 3, 3)], base + 12)
        self.second = Gather(place, block.ring1, lambda j, h: held.at[j, 12 * h:12 * h + 12], base + 18)

    def piece(self, a1, a2, q, m):
        return self.held.at[a1, (2 * a2 + q) * 3 + m]

    def parts(self, dz):
        bk = self.bk
        target = (bk.t + dz) % 4
        core = bk.t // 2
        a1, a2 = bk.order(bk.w, bk.x, core)
        for m in range(2):
            whole = self.piece(a1, a2, bk.t % 2, m)
            copies = [(self.shards[m].at[:, src], whole.at[:, dst]) for src, dst in bk.pieces(target)]
            yield m, copies, whole, bk.dev(target, bk.w, bk.x, core)

    def out_part(self, core):
        a1, a2 = self.bk.order(self.bk.w, self.bk.x, core)
        copies = [(self.shards[2].at[2 * core + q], self.piece(a1, a2, q, 2)) for q in range(2)]
        return copies, self.held.at[a1, pl.ds(0, 2)]

    def source(self, wait):
        place, s = self.pl, self.s
        mine = self.bk.t // 2 == s

        def away(copies, whole, dev, slot):
            if wait:
                place.remote(whole, whole, dev, slot).wait_send()
                return
            for src, dst in copies:
                place.remote(src, dst, dev, slot).start()

        def here(copies, whole, slot):
            if wait:
                place.local(whole, whole, slot).wait()
                return
            for src, dst in copies:
                place.local(src, dst, slot).start()

        @pl.when(place.c == s)
        def _():
            for dz in range(1, 4):
                for m, copies, whole, dev in self.parts(dz):
                    away(copies, whole, dev, self.slots + 2 * dz + m)

            @pl.when(mine)
            def _():
                for m, copies, whole, _ in self.parts(0):
                    here(copies, whole, self.local + m)

            @pl.when(jnp.logical_not(mine))
            def _():
                for m, copies, whole, _ in self.parts(0):
                    away(copies, whole, place.partner, self.slots + m)
            here(*self.out_part(s), self.local + 2)
            away(*self.out_part(1 - s), place.partner, self.out_slot)

    def send(self):
        self.source(False)

    def arrive(self):
        place, bk, s = self.pl, self.bk, self.s
        for dz in range(4):
            source = (bk.t + 4 - dz) % 4
            here = source // 2 == place.c
            if dz == 0:
                here = jnp.logical_and(here, place.c != s)

            @pl.when(here)
            def _(dz=dz, source=source):
                for m in range(2):
                    dst = self.piece(bk.a1, bk.a2, source % 2, m)
                    place.remote(dst, dst, place.partner, self.slots + 2 * dz + m).wait_recv()

        self.source(True)

        @pl.when(place.c != s)
        def _():
            _, whole = self.out_part(1 - s)
            place.remote(whole, whole, place.partner, self.out_slot).wait_recv()

    def spread(self, a1):
        place, bk = self.pl, self.bk

        def one(a2):
            w, x = bk.place(a1, a2, place.c)
            for m in range(3):
                for q in range(2):
                    src = self.piece(a1, a2, q, m)
                    dst = self.outs[m].at[bk.index(m, w, x, 2 * place.c + q)]
                    place.remote(src, dst, place.partner, self.swap_slots + m).start()
                    place.local(src, dst, self.copy_local + m).start()
        loop(4, one)

    def done(self):
        place, bk = self.pl, self.bk
        every = slice(None)
        for m in range(3):
            mine, other = (self.outs[m].at[bk.index(m, every, every, pair(core))] for core in (place.c, 1 - place.c))
            place.remote(mine, other, place.partner, self.swap_slots + m).wait_recv()
            place.remote(mine, other, place.partner, self.swap_slots + m).wait_send()
            place.local(mine, mine, self.copy_local + m).wait()

    def step1(self):
        self.arrive()
        self.first.start()

    def step2(self):
        self.first.relay()

    def step3(self):
        self.first.finish()
        self.second.start()
        self.spread(self.bk.a1)

    def step4(self):
        self.second.relay()

    def step5(self):
        self.second.near()
        self.spread((self.bk.a1 + 3) % 4)
        self.spread((self.bk.a1 + 1) % 4)

    def step6(self):
        self.second.far()
        self.spread((self.bk.a1 + 2) % 4)


class Grads:
    def __init__(self, place, block, m, part, kit, out, base, local):
        self.pl, self.bk, self.s, self.m, self.part, self.out = place, block, block.b, m, part, out
        mine, held1, held2, sum2 = kit
        self.mine, self.held1, self.held2, self.sum2 = mine, held1, held2, sum2
        self.local = local
        self.swap_slot, self.hand_slots = base, base + 1

        def add1(h, j):
            def one(i):
                k, q = i // 2, i % 2
                held1[0, h, k, q] = held1[0, h, k, q] + mine[j, 2 * h + k, q]
            loop(4, one)
        self.first = Reduce(place, block.ring1, lambda j, h: mine.at[j, 2 * h:2 * h + 2], lambda b: held1.at[b], add1, base + 5)

        def add2(h, j):
            held2[0, h] = held2[0, h] + mine[block.a1, j, h]
        self.second = Reduce(place, block.ring2, lambda j, h: mine.at[block.a1, j, h], lambda b: held2.at[b], add2, base + 11)

    def swap(self):
        place, bk = self.pl, self.bk

        def one(p):
            w, x, other = p // 4, p % 4, 1 - place.c
            a1, a2 = bk.order(w, x, other)
            src = self.part.at[bk.index(self.m, w, x, pair(other))]
            place.remote(src, self.mine.at[a1, a2], place.partner, self.swap_slot).start()
        loop(16, one)

    def combine(self):
        place, bk, mine = self.pl, self.bk, self.mine
        whole = place.remote(mine, mine, place.partner, self.swap_slot)
        whole.wait_recv()

        def one(p):
            w, x = p // 4, p % 4
            a1, a2 = bk.order(w, x, place.c)
            for q in range(2):
                mine[a1, a2, q] = mine[a1, a2, q] + self.part[bk.index(self.m, w, x, 2 * place.c + q)]
        loop(16, one)
        whole.wait_send()

    def turn(self):
        bk, mine, held1 = self.bk, self.mine, self.held1
        self.first.finish()

        def one(i):
            h, k, q = i // 4, i // 2 % 2, i % 2
            mine[bk.a1, i // 2, q] = mine[bk.a1, i // 2, q] + held1[1, h, k, q] + held1[2, h, k, q]
        loop(8, one)
        self.second.start()

    def last(self):
        self.second.finish()
        for h in range(2):
            self.sum2[h] = self.mine[self.bk.a1, self.bk.a2, h] + self.held2[1, h] + self.held2[2, h]
        self.hand(False)

    def hand(self, wait):
        place, bk, s = self.pl, self.bk, self.s
        to_self = place.c == s

        def stay(copies, whole):
            if wait:
                place.local(whole, whole, self.local).wait()
                return
            for src, dst in copies:
                place.local(src, dst, self.local).start()

        def go(copies, whole, dev, slot):
            if wait:
                place.remote(whole, whole, dev, slot).wait_send()
                return
            for src, dst in copies:
                place.remote(src, dst, dev, slot).start()

        if self.m == 2:
            copies = [(self.sum2, self.out.at[pair(place.c)])]
            pl.when(to_self)(lambda: stay(copies, self.sum2))
            pl.when(jnp.logical_not(to_self))(lambda: go(copies, self.sum2, place.partner, self.hand_slots))
            return
        for dz in range(4):
            target = (bk.t + dz) % 4
            whole = self.sum2.at[target % 2]
            copies = [(self.sum2.at[target % 2, :, own], self.out.at[:, shard]) for shard, own in bk.pieces(bk.t)]
            here = target // 2 == place.c
            send = functools.partial(go, copies, whole, bk.dev(target, bk.w, bk.x, s), self.hand_slots + dz)
            if dz:
                pl.when(here)(send)
            else:
                pl.when(jnp.logical_and(here, to_self))(functools.partial(stay, copies, whole))
                pl.when(jnp.logical_and(here, jnp.logical_not(to_self)))(send)

    def done(self):
        place, bk, s = self.pl, self.bk, self.s

        def land(like, slot):
            place.remote(like, like, place.partner, slot).wait_recv()

        @pl.when(place.c == s)
        def _():
            if self.m == 2:
                land(self.sum2, self.hand_slots)
                return
            for dz in range(1, 4):
                land(self.sum2.at[0], self.hand_slots + dz)
            pl.when(bk.t // 2 != s)(lambda: land(self.sum2.at[0], self.hand_slots))
        self.hand(True)


def mm(a, b):
    return jnp.dot(a, b, preferred_element_type=F32)


def mm_nt(a, b):
    return lax.dot_general(a, b, (((1,), (1,)), ((), ())), preferred_element_type=F32)


def mm_tn(a, b):
    return lax.dot_general(a, b, (((0,), (0,)), ((), ())), preferred_element_type=F32)


def chunk(ref, k):
    return ref[k].reshape(ROWS, WIDE)


def square(ref):
    return ref[...].reshape(WIDE, WIDE)


def pre_acts(n_ref, k, gate, inn, a_ref, b_ref, slot):
    a_ref[slot] = mm(chunk(n_ref, k), square(gate))
    b_ref[slot] = mm(chunk(n_ref, k), square(inn))


def hidden(a_ref, b_ref, slot, u_ref, k):
    def one(i):
        rows = pl.ds(pl.multiple_of(i * STEP, STEP), STEP)
        a = a_ref[slot, rows]
        u_ref[k, rows] = (a * jax.nn.sigmoid(a) * b_ref[slot, rows]).astype(BF16)
    loop(ROWS // STEP, one)


def project(u_ref, k, out, part):
    part[k] = mm(u_ref[k], square(out)).reshape(4, 2, HALF, WIDE)


def hidden_back(e_ref, k, out, t_ref, a_ref, b_ref, slot, dab):
    t_ref[k] = mm_nt(chunk(e_ref, k), square(out)).reshape(4, 2, HALF, WIDE)
    per_half = HALF // STEP

    def one(i):
        rows = pl.ds(pl.multiple_of(i * STEP, STEP), STEP)
        j = i // (2 * per_half)
        h = i // per_half % 2
        t = t_ref[k, j, h, pl.ds(pl.multiple_of(i % per_half * STEP, STEP), STEP)]
        a, b = a_ref[slot, rows], b_ref[slot, rows]
        s = jax.nn.sigmoid(a)
        dab[k, i] = (t * b * s * (1.0 + a * (1.0 - s))).astype(BF16)
        dab[k, GROUPS + i] = (t * a * s).astype(BF16)
    loop(ROWS // STEP, one)


def input_back(dab, k, gate, inn, part):
    def one(i):
        da, db = dab[k, :GROUPS].reshape(ROWS, WIDE), dab[k, GROUPS:].reshape(ROWS, WIDE)
        cols = pl.ds(pl.multiple_of(i * COLS, COLS), COLS)
        dn = mm_nt(da, gate[pl.ds(2 * i, 2)].reshape(COLS, WIDE)) + mm_nt(db, inn[pl.ds(2 * i, 2)].reshape(COLS, WIDE))
        part[k, :, :, :, cols] = dn.reshape(4, 2, HALF, COLS)
    loop(WIDE // COLS, one)


def weight_grad(lhs, rhs, out):
    def one(i):
        cols = pl.ds(pl.multiple_of(i * 256, 256), 256)
        left = lhs[..., cols].reshape(CHUNKS * ROWS, 256)
        out[i] = mm_tn(left, rhs[...].reshape(CHUNKS * ROWS, WIDE)).reshape(4, 4, 16, WIDE)
    loop(4, one)


def weight_grad_of(n_ref, dab, first, out):
    def one(i):
        cols = pl.ds(pl.multiple_of(i * 256, 256), 256)
        right = dab[:, first:first + GROUPS].reshape(CHUNKS * ROWS, WIDE)
        out[i] = mm_tn(n_ref[..., cols].reshape(CHUNKS * ROWS, 256), right).reshape(4, 4, 16, WIDE)
    loop(4, one)


HEAVY = {'w0': 'split', 'w1': 'x', 'v0': 'x', 'out1': 'x', 'gate1': 'split', 'in1': 'split', 'out0': 'split', 'gate0': 'split', 'in0': 'split'}


def kernel(x_in, g_in, wg, wi, wo, dx_out, gg, gi, go, a_out, b_out, u_out, n_out, held_1, held_0,
           xs, hs, n0e, n1, ga, u_s, a_s, b_s, dab, part, held, w0g, w0i, w0o, w1g, w1i, w1o,
           d_a, d_b, mine, held1, held2, sum2, ssem, rsem, lsem, phase):
    place = Place(ssem, rsem, lsem, phase)
    z, y, c = place.z, place.y, place.c
    rows0, rows1 = Block(place, 0, 'x').rows, Block(place, 1, 'x').rows
    per_row = 6 * CHUNKS
    z_gather, z_sum, g_gather, y_gather, y_sum = (place.slots(per_row) for _ in range(5))
    n0, e = (Spreads(place, rows0, n0e, z_gather) for _ in range(2))
    o, d0 = (Rows(place, rows0, part, held, z_sum) for _ in range(2))
    g = Spreads(place, rows1, ga, g_gather)
    n = Spreads(place, rows1, n1, y_gather)
    d1 = Rows(place, rows1, part, held, y_sum)
    shards = (wg, wi, wo)
    w0_slots, w0_local = place.slots(24), place.local_slots(6)
    w0 = Weights(place, Block(place, 0, HEAVY['w0']), shards, dab, (w0g, w0i, w0o), w0_slots, w0_local)
    v0 = Weights(place, Block(place, 0, HEAVY['v0']), shards, held_0, (w0g, w0i, w0o), w0_slots, w0_local)
    w1 = Weights(place, Block(place, 1, HEAVY['w1']), shards, held_1, (w1g, w1i, w1o), place.slots(24), place.local_slots(6))
    outs = gg, gi, go

    def grads(b, m, part, own, ring):
        name = ('gate', 'in', 'out')[m] + str(b)
        kit = mine.at[own], held1.at[ring], held2.at[own], sum2.at[own]
        return Grads(place, Block(place, b, HEAVY[name]), m, part, kit, outs[m], place.slots(17), place.local_slots(1))
    out1, gate1, inn1 = grads(1, 2, d_a, 0, 0), grads(1, 0, d_b, 1, 1), grads(1, 1, d_a, 2, 2)
    out0, gate0, inn0 = grads(0, 2, d_b, 3, 3), grads(0, 0, d_a, 4, 0), grads(0, 1, d_b, 0, 1)
    x_copy = place.local(x_in.at[c], xs, place.local_slots(1))
    g_copy = place.local(g_in.at[c], ga.at[:, y], place.local_slots(1))
    save = place.local_slots(8)
    n_save, n_load = place.local(n0e, n_out, save + 6), place.local(n_out, n1, save + 6)
    u_load = place.local(u_out, u_s, save + 7)

    def saves(k):
        slot = k % 2
        at = save + 3 * slot
        return place.local(a_s.at[slot], a_out.at[k], at), place.local(b_s.at[slot], b_out.at[k], at + 1), place.local(u_s.at[k], u_out.at[k], at + 2)

    def loads(k):
        slot = k % 2
        at = save + 3 * slot
        return place.local(a_out.at[k], a_s.at[slot], at), place.local(b_out.at[k], b_s.at[slot], at + 1)

    def start(copies):
        for copy in copies:
            copy.start()

    def wait(copies):
        for copy in copies:
            copy.wait()

    def forward(k):
        if k >= 2:
            wait(saves(k - 2))
        pre_acts(n0e, k, w0g, w0i, a_s, b_s, k % 2)
        hidden(a_s, b_s, k % 2, u_s, k)
        start(saves(k))
        project(u_s, k, w0o, part)

    def close_o(k):
        o(k).finish()

        def step(h, rows):
            total = o.total(k, h, rows).astype(BF16).astype(F32)
            out = (xs[k, h, rows].astype(F32) + total).astype(BF16)
            hs[k, h, rows] = out
            n1[k, y, h, rows] = rms(out.astype(F32))
        by_rows(step)
        n(k).start()

    def middle(k):
        n(k).finish()
        pre_acts(n1, k, w1g, w1i, a_s, b_s, k % 2)
        hidden(a_s, b_s, k % 2, u_s, k)
        hidden_back(ga, k, w1o, part, a_s, b_s, k % 2, dab)
        input_back(dab, k, w1g, w1i, part)

    def close_1(k):
        d1(k).finish()

        def step(h, rows):
            dn = d1.total(k, h, rows)
            n0e[k, z, h, rows] = cotangent(hs[k, h, rows].astype(F32), ga[k, y, h, rows].astype(F32), dn)
        by_rows(step)
        e(k).start()

    def back_hidden(k):
        e(k).finish()
        wait(loads(k))
        hidden_back(n0e, k, w0o, part, a_s, b_s, k % 2, dab)
        if k < 2:
            start(loads(k + 2))

    def back_input(k):
        input_back(dab, k, w0g, w0i, part)
        d0(k).start()

    def close_0(k):
        d0(k).finish()

        def step(h, rows):
            dn = d0.total(k, h, rows)
            hs[k, h, rows] = cotangent(xs[k, h, rows].astype(F32), n0e[k, z, h, rows].astype(F32), dn)
        by_rows(step)

    x_copy.start()
    g_copy.start()
    barrier = pltpu.get_barrier_semaphore()
    place.signal(barrier)
    place.wait(barrier)
    w0.send()
    w1.send()
    x_copy.wait()

    def start_n0(k):
        def norm(h, rows):
            n0e[k, z, h, rows] = rms(xs[k, h, rows].astype(F32))
        by_rows(norm)
        n0(k).start()
    loop(CHUNKS, start_n0)
    w0.step1()
    n0(0).relay()
    w0.step2()
    n0(1).relay()
    w0.step3()
    n0(2).relay()
    n0(3).relay()
    w1.step1()
    w0.step4()
    loop(CHUNKS, lambda k: n0(k).finish())
    n_save.start()
    w1.step2()
    w0.step5()
    g_copy.wait()
    loop(CHUNKS, lambda k: g(k).start())
    w1.step3()
    w0.step6()
    w0.done()

    forward(0)
    o(0).start()
    forward(1)
    g(0).relay()
    g(1).relay()
    o(0).relay()
    o(1).start()
    forward(2)
    g(2).relay()
    w1.step4()
    g(3).relay()
    close_o(0)
    o(1).relay()
    o(2).start()
    n(0).relay()
    w1.step5()
    forward(3)
    n_save.wait()
    place.signal(phase.at[0])
    v0.send()
    o(2).relay()
    o(3).start()
    loop(CHUNKS, lambda k: g(k).finish())
    wait(saves(2))
    wait(saves(3))
    w1.step6()
    close_o(1)
    w1.done()

    middle(0)
    n(1).relay()
    d1(0).start()
    o(3).relay()
    v0.step1()
    close_o(2)
    middle(1)
    n(2).relay()
    d1(0).relay()
    d1(1).start()
    v0.step2()
    close_o(3)
    middle(2)
    n(3).relay()
    d1(1).relay()
    d1(2).start()
    place.wait(phase.at[0])
    v0.step3()
    start(loads(0))
    close_1(0)
    middle(3)
    d1(2).relay()
    d1(3).start()
    start(loads(1))
    e(0).relay()
    v0.step4()
    weight_grad(u_s, ga, d_a)
    out1.swap()
    u_load.start()
    close_1(1)
    weight_grad_of(n1, dab, 0, d_b)
    gate1.swap()
    d1(3).relay()
    v0.step5()
    out1.combine()
    out1.first.start()
    e(1).relay()
    weight_grad_of(n1, dab, GROUPS, d_a)
    inn1.swap()
    n_load.start()
    close_1(2)
    gate1.combine()
    v0.step6()
    close_1(3)
    v0.done()

    e(2).relay()
    back_hidden(0)
    e(3).relay()
    inn1.combine()
    gate1.first.start()
    back_hidden(1)
    out1.first.relay()
    back_hidden(2)
    u_load.wait()
    n_load.wait()
    inn1.first.start()
    e(3).finish()
    weight_grad(u_s, n0e, d_b)
    out0.swap()
    gate1.first.relay()
    wait(loads(3))
    hidden_back(n0e, 3, w0o, part, a_s, b_s, 1, dab)
    out1.turn()
    place.signal(phase.at[1])
    weight_grad_of(n1, dab, 0, d_a)
    out0.combine()
    out0.first.start()
    place.wait(phase.at[1])
    gate0.swap()
    back_input(0)
    inn1.first.relay()
    weight_grad_of(n1, dab, GROUPS, d_b)
    gate0.combine()
    gate0.first.start()
    out1.second.relay()
    back_input(1)
    d0(0).relay()
    gate1.turn()
    out1.last()
    out1.done()
    place.signal(phase.at[2])
    out0.first.relay()
    back_input(2)
    place.wait(phase.at[2])
    inn0.swap()
    d0(1).relay()
    gate1.second.relay()
    inn0.combine()
    inn0.first.start()
    back_input(3)
    inn1.turn()
    d0(2).relay()
    gate0.first.relay()
    out0.turn()
    gate1.last()
    inn1.second.relay()
    close_0(0)
    d0(3).relay()
    inn0.first.relay()
    out0.second.relay()
    gate0.turn()
    inn1.last()
    close_0(1)
    close_0(2)
    gate0.second.relay()
    out0.last()
    close_0(3)
    dx_slot, dx_local = place.slots(1), place.local_slots(1)
    dx_away, dx_here = place.remote(hs, dx_out.at[c], place.partner, dx_slot), place.local(hs, dx_out.at[c], dx_local)
    dx_away.start()
    dx_here.start()
    inn0.turn()
    gate0.last()
    gate1.done()
    inn1.done()
    inn0.second.relay()
    inn0.last()
    dx_away.wait()
    dx_here.wait()
    out0.done()
    gate0.done()
    inn0.done()


VM = pl.BlockSpec(memory_space=pltpu.VMEM)
ANY = pl.BlockSpec(memory_space=pl.ANY)


def sds(shape, dtype):
    return jax.ShapeDtypeStruct(shape, dtype)


ALL_ROWS = (CHUNKS, 4, 2, HALF, WIDE)
OWN_ROWS = (CHUNKS, 2, HALF, WIDE)
FLAT_ROWS = (CHUNKS, ROWS, WIDE)
WEIGHT = (4, 4, 4, 16, WIDE)
STAGED = (4, 24, 16, WIDE)
OUTS = [
    sds((2,) + OWN_ROWS, BF16), sds((16, 4 * WIDE), F32), sds((16, 4 * WIDE), F32), sds((4, 16, WIDE), F32),
    sds(FLAT_ROWS, F32), sds(FLAT_ROWS, F32), sds(FLAT_ROWS, BF16), sds(ALL_ROWS, BF16),
    sds(STAGED, BF16), sds(STAGED, BF16),
]
SCRATCH = (
    [pltpu.VMEM(OWN_ROWS, BF16)] * 2
    + [pltpu.VMEM(ALL_ROWS, BF16)] * 3
    + [pltpu.VMEM(FLAT_ROWS, BF16)]
    + [pltpu.VMEM((2, ROWS, WIDE), F32)] * 2
    + [pltpu.VMEM((CHUNKS, 2 * GROUPS, STEP, WIDE), BF16)]
    + [pltpu.VMEM(ALL_ROWS, F32), pltpu.VMEM((3,) + OWN_ROWS, F32)]
    + [pltpu.VMEM(WEIGHT, BF16)] * 6
    + [pltpu.VMEM(WEIGHT, F32)] * 2
    + [
        pltpu.VMEM((5, 4, 4, 2, 16, WIDE), F32),
        pltpu.VMEM((4, 3, 2, 2, 2, 16, WIDE), F32),
        pltpu.VMEM((5, 3, 2, 16, WIDE), F32),
        pltpu.VMEM((5, 2, 16, WIDE), F32),
    ]
    + [pltpu.SemaphoreType.DMA((N_REMOTE,)), pltpu.SemaphoreType.DMA((N_REMOTE,)), pltpu.SemaphoreType.DMA((N_LOCAL,))]
    + [pltpu.SemaphoreType.REGULAR((3,))]
)


def call(*operands):
    return pl.pallas_call(
        kernel,
        out_shape=OUTS,
        in_specs=[ANY] * 2 + [VM] * 3,
        out_specs=[ANY] * len(OUTS),
        scratch_shapes=SCRATCH,
        compiler_params=pltpu.CompilerParams(collective_id=1, has_side_effects=True, vmem_limit_bytes=67043328),
        name='kernel_all',
    )(*operands)


def solution(mesh):
    act_spec = P(None, 'data', None, None)
    weight_spec = P('stage', None, 'data', None)

    def per_device(x, g, w_gate, w_in, w_out):
        shards = (w_gate.reshape(16, 4 * WIDE), w_in.reshape(16, 4 * WIDE), w_out.reshape(4, 16, WIDE))
        dx, d_gate, d_in, d_out, *_ = call(x.reshape((2,) + OWN_ROWS), g.reshape((2,) + OWN_ROWS), *shards)
        return dx.reshape(x.shape), d_gate.reshape(w_gate.shape), d_in.reshape(w_in.shape), d_out.reshape(w_out.shape)

    return jax.shard_map(per_device, mesh=mesh, in_specs=(act_spec, act_spec, weight_spec, weight_spec, weight_spec), out_specs=(act_spec, weight_spec, weight_spec, weight_spec), check_vma=False)
```
